32 devices in a mesh: seq: 8 (over y, x, core), head: 4 (over z).
Axes of the slice: x: 2, y: 2, z: 4, core: 2. Of those that a mesh axis runs over, the one named last changes fastest.
Arguments:
- values: bfloat16 [4096, 8192], P('seq', 'head'), may hold values from -6 to 6
- group_keys: bfloat16 [4096, 8, 128], P(('seq', 'head')), may hold values from -0.5 to 0.5
- group_queries: bfloat16 [4096, 8, 128], P(('seq', 'head')), may hold values from -0.16992188 to 0.16992188
- level_table: int32 [128, 20], P('head'), may hold values from 1 to 4
- window_index: int32 [1], replicated, may hold values from 0 to 15
- prior_states: bfloat16 [4, 128, 64, 128], P(None, 'head'), may hold values from -100 to 100
- cotangent: bfloat16 [4096, 8192], P('seq', 'head'), may hold values from -6 to 6
Outputs:
- mixer_out: bfloat16 [4096, 8192], P('seq', 'head')
- grad_values: bfloat16 [4096, 8192], P('seq', 'head')
- grad_keys: float32 [4096, 8, 128], P(('seq', 'head'))
- grad_queries: float32 [4096, 8, 128], P(('seq', 'head'))
- grad_prior: float32 [4, 128, 64, 128], P(None, 'head')
The draws below stay inside these ranges and needn't reach their ends.
All inputs are finite; a program needn't handle non-finite values.
Results may differ from the reference program's by a relative error of at most 0.015.
Values may be sent and summed in bfloat16 or wider, within the bound.
No kernel may reach another device: no remote copies, remote signals or barrier semaphores. Data moves between devices by JAX's collectives and lax.ppermute only.
A program may use at most 128 MiB of HBM per device.

```python
import jax
import jax.numpy as jnp
from jax import lax

HEADS = 128
HEAD_DIM = 64
STATE = 128
GROUPS = 8
LEVELS = 20
PLEVELS = 4
TOK_DEV = 512
TOKENS = 4096
N_SEQ = 8


def plant(array, rng, smallest, largest):
    place = [jax.random.randint(jax.random.fold_in(rng, axis), (), 0, length) for axis, length in enumerate(array.shape)]
    main_axis = array.shape.index(max(array.shape))
    next_to = place[:main_axis] + [(place[main_axis] + 1) % array.shape[main_axis]] + place[main_axis + 1:]
    return array.at[tuple(place)].set(smallest).at[tuple(next_to)].set(largest)


def block_scale(stream_key, shape, shards, low, largest):
    gain = 1.0
    for dim, shards_of in shards:
        steps = jax.random.uniform(jax.random.fold_in(jax.random.fold_in(stream_key, 6), dim), (shards_of,), jnp.float32, low / len(shards), largest / len(shards))
        gain = gain * jnp.repeat(jnp.exp(steps), shape[dim] // shards_of).reshape((-1,) + (1,) * (len(shape) - 1 - dim))
    return gain


def centred(key, shape, width, bound, split=(), held_as=jnp.bfloat16):
    level = block_scale(key, shape, split, -0.22, 0.18) if split else 1.0
    values = jax.random.normal(key, shape, jnp.float32) * width * level
    return jnp.minimum(jnp.maximum(values, -bound), bound).astype(held_as)


def setup_inputs(seed: int = 0) -> dict:
    streams_of = jax.random.split(jax.random.key(seed), 8)
    return {
        "values": centred(streams_of[0], (TOKENS, HEADS * HEAD_DIM), 1.0, 6.0, ((0, 8), (1, 4))),
        "group_keys": jnp.clip(jax.random.uniform(streams_of[1], (TOKENS, GROUPS, STATE), jnp.float32, -0.5, 0.5) * block_scale(streams_of[1], (TOKENS, GROUPS, STATE), ((0, 32),), -0.4, 0.0), -0.5, 0.5).astype(jnp.bfloat16),
        "group_queries": jnp.clip(jax.random.uniform(streams_of[2], (TOKENS, GROUPS, STATE), jnp.float32, -0.16992188, 0.16992188) * block_scale(streams_of[2], (TOKENS, GROUPS, STATE), ((0, 32),), -0.4, 0.0), -0.16992188, 0.16992188).astype(jnp.bfloat16),
        "level_table": plant(jax.random.randint(streams_of[3], (HEADS, LEVELS), 1, 5), jax.random.fold_in(streams_of[3], 1), 1, 4).astype(jnp.int32),
        "window_index": jax.random.randint(streams_of[4], (1,), 0, 2 ** PLEVELS).astype(jnp.int32),
        "prior_states": jnp.clip(jax.random.uniform(streams_of[5], (PLEVELS, HEADS, HEAD_DIM, STATE), jnp.float32, -100.0, 100.0) * block_scale(streams_of[5], (PLEVELS, HEADS, HEAD_DIM, STATE), ((1, 4),), -0.4, 0.0), -100.0, 100.0).astype(jnp.bfloat16),
        "cotangent": centred(streams_of[6], (TOKENS, HEADS * HEAD_DIM), 0.5, 6.0, ((0, 8), (1, 4))),
    }


def level_weights(level_table):
    level_count = level_table.shape[1]
    exponent = jnp.maximum(jnp.arange(level_count, dtype=jnp.float32) - 1.0, 0.0) * 0.5
    return level_table.astype(jnp.float32) * jnp.exp2(-exponent)


def highest_bit(numbers, bit_count):
    result = jnp.zeros(numbers.shape, jnp.int32)
    for bit_shift in range(1, bit_count):
        result = result + (numbers >= (1 << bit_shift)).astype(jnp.int32)
    return result


def reference(values, group_keys, group_queries, level_table, window_index, prior_states, cotangent):
    highest = lax.Precision.HIGHEST
    log_rows = TOK_DEV.bit_length() - 1
    log_seq = N_SEQ.bit_length() - 1
    log_window = log_rows + log_seq
    per_group = HEADS // GROUPS
    weights = level_weights(level_table)
    value_view = values.reshape(N_SEQ, TOK_DEV, GROUPS, per_group, HEAD_DIM)
    cot_view = cotangent.reshape(N_SEQ, TOK_DEV, GROUPS, per_group, HEAD_DIM)
    key_view = group_keys.reshape(N_SEQ, TOK_DEV, GROUPS, STATE)
    query_view = group_queries.reshape(N_SEQ, TOK_DEV, GROUPS, STATE)

    def segment_states(operands):
        value_seg, key_seg = operands
        outer = jnp.einsum("tgkp,tgn->gkpn", value_seg.astype(jnp.float32), key_seg.astype(jnp.float32), precision=highest)
        return outer.reshape(HEADS, HEAD_DIM, STATE).astype(jnp.bfloat16)

    states = lax.map(segment_states, (value_view, key_view))
    adjoints = lax.map(segment_states, (cot_view, query_view))
    segments = jnp.arange(N_SEQ, dtype=jnp.int32)
    seg_levels = 1 + log_rows + highest_bit(jnp.bitwise_xor(segments[:, None], segments[None, :]), log_seq)
    pair_weights = jnp.where((segments[None, :] < segments[:, None])[None], weights[:, seg_levels], 0.0)
    inflow = jnp.einsum("hij,jhpn->ihpn", pair_weights, states.astype(jnp.float32), precision=highest)
    outflow = jnp.einsum("hij,ihpn->jhpn", pair_weights, adjoints.astype(jnp.float32), precision=highest)
    window_bits = ((window_index[0] >> jnp.arange(PLEVELS, dtype=jnp.int32)) & 1).astype(jnp.float32)
    prior_weights = weights[:, 1 + log_window:1 + log_window + PLEVELS] * window_bits[None, :]
    prior_term = jnp.einsum("hk,khpn->hpn", prior_weights, prior_states.astype(jnp.float32), precision=highest)
    inflow_cast = (inflow + prior_term[None]).astype(jnp.bfloat16)
    outflow_cast = outflow.astype(jnp.bfloat16)
    grand_total = jnp.sum(adjoints.astype(jnp.float32), axis=0)
    grad_prior = prior_weights.T[:, :, None, None] * grand_total[None]

    positions = jnp.arange(TOK_DEV, dtype=jnp.int32)
    spread = jnp.bitwise_xor(positions[:, None], positions[None, :])
    level_grid = jnp.where(spread == 0, 0, 1 + highest_bit(spread, log_rows))
    causal = positions[:, None] >= positions[None, :]
    group_weights = weights.reshape(GROUPS, per_group, LEVELS)
    inflow_groups = inflow_cast.reshape(N_SEQ, GROUPS, per_group, HEAD_DIM, STATE)
    outflow_groups = outflow_cast.reshape(N_SEQ, GROUPS, per_group, HEAD_DIM, STATE)

    def one_group(operands):
        value_grp, cot_grp, key_grp, query_grp, inflow_grp, outflow_grp, weight_grp = operands
        factor_grid = jnp.where(causal[None], weight_grp[:, level_grid], 0.0)
        scores = jnp.dot(query_grp, key_grp.T, preferred_element_type=jnp.float32)
        weighted = (factor_grid * scores[None]).astype(jnp.bfloat16)
        weighted_wide = weighted.astype(jnp.float32)
        value_wide = value_grp.astype(jnp.float32)
        cot_wide = cot_grp.astype(jnp.float32)
        key_wide = key_grp.astype(jnp.float32)
        query_wide = query_grp.astype(jnp.float32)
        inflow_wide = inflow_grp.astype(jnp.float32)
        outflow_wide = outflow_grp.astype(jnp.float32)
        mixer_rows = jnp.einsum("hts,shp->thp", weighted_wide, value_wide, precision=highest)
        mixer_rows = mixer_rows + jnp.einsum("tn,hpn->thp", query_wide, inflow_wide, precision=highest)
        grad_raw = jnp.einsum("thp,shp->hts", cot_wide, value_wide, precision=highest)
        grad_weighted = (factor_grid * grad_raw).astype(jnp.bfloat16).astype(jnp.float32)
        value_grad = jnp.einsum("hts,thp->shp", weighted_wide, cot_wide, precision=highest)
        value_grad = value_grad + jnp.einsum("sn,hpn->shp", key_wide, outflow_wide, precision=highest)
        query_grad = jnp.einsum("hts,sn->tn", grad_weighted, key_wide, precision=highest)
        query_grad = query_grad + jnp.einsum("thp,hpn->tn", cot_wide, inflow_wide, precision=highest)
        key_grad = jnp.einsum("hts,tn->sn", grad_weighted, query_wide, precision=highest)
        key_grad = key_grad + jnp.einsum("shp,hpn->sn", value_wide, outflow_wide, precision=highest)
        return mixer_rows.astype(jnp.bfloat16), value_grad.astype(jnp.bfloat16), query_grad, key_grad

    def one_segment(operands):
        value_seg, cot_seg, key_seg, query_seg, inflow_seg, outflow_seg = operands
        return lax.map(one_group, (jnp.moveaxis(value_seg, 1, 0), jnp.moveaxis(cot_seg, 1, 0), jnp.moveaxis(key_seg, 1, 0), jnp.moveaxis(query_seg, 1, 0), inflow_seg, outflow_seg, group_weights))

    mixer_all, value_all, query_all, key_all = lax.map(one_segment, (value_view, cot_view, key_view, query_view, inflow_groups, outflow_groups))
    mixer_out = jnp.transpose(mixer_all, (0, 2, 1, 3, 4)).reshape(TOKENS, HEADS * HEAD_DIM)
    grad_values = jnp.transpose(value_all, (0, 2, 1, 3, 4)).reshape(TOKENS, HEADS * HEAD_DIM)
    grad_queries = jnp.transpose(query_all, (0, 2, 1, 3)).reshape(TOKENS, GROUPS, STATE)
    grad_keys = jnp.transpose(key_all, (0, 2, 1, 3)).reshape(TOKENS, GROUPS, STATE)
    return mixer_out, grad_values, grad_keys, grad_queries, grad_prior
```

```python
import functools

import jax
import jax.numpy as jnp
from jax import lax
from jax.experimental import pallas as pl
from jax.experimental.pallas import tpu as pltpu
from jax.sharding import PartitionSpec as P

HEADS = 128
GROUPS = 8
BF = jnp.bfloat16
F32 = jnp.float32


def partner_2(array, axis, apart):
    return lax.ppermute(array, axis, [(i, i ^ 1 << apart) for i in range(lax.axis_size(axis))])


def level_weights(level_table):
    level_count = level_table.shape[1]
    exponent = jnp.maximum(jnp.arange(level_count, dtype=F32) - 1.0, 0.0) * 0.5
    return level_table.astype(F32) * jnp.exp2(-exponent)


def dot_nn(a, b):
    return lax.dot_general(a, b, (((1,), (0,)), ((), ())), preferred_element_type=F32)


def dot_nt(a, b):
    return lax.dot_general(a, b, (((1,), (1,)), ((), ())), preferred_element_type=F32)


def dot_tn(a, b):
    return lax.dot_general(a, b, (((0,), (0,)), ((), ())), preferred_element_type=F32)


def states_kernel(x_ref, r_ref, o_ref):
    o_ref[...] = dot_tn(x_ref[...], r_ref[...]).astype(o_ref.dtype)


def block_states(x, rows, cols, per_group):
    tok, width = x.shape
    state = 128
    return pl.pallas_call(
        states_kernel,
        grid=(width // cols,),
        in_specs=[
            pl.BlockSpec((tok, cols), lambda i: (0, i)),
            pl.BlockSpec((tok, state), lambda i: (0, i // per_group)),
        ],
        out_specs=pl.BlockSpec((cols, state), lambda i: (i, 0)),
        out_shape=jax.ShapeDtypeStruct((width, state), BF),
        cost_estimate=pl.CostEstimate(
            flops=2 * tok * width * state, transcendentals=0, bytes_accessed=2 * tok * width
        ),
        name="states",
    )(x, rows)


def intra_kernel(
    w_ref, cw_ref, v_ref, c_ref, k_ref, q_ref,
    mix_ref, dv_ref, qg_ref, kg_ref,
    s_sc, st_sc, sb_sc, stb_sc, g_sc,
    *, base, head_dim,
):
    tok, cols = v_ref.shape
    blocks = tok // base
    log_base = base.bit_length() - 1
    log_blocks = blocks.bit_length() - 1
    heads = cols // head_dim
    step = pl.program_id(1)
    first_head = (pl.program_id(0) * pl.num_programs(1) + step) * heads
    rows_i = lax.broadcasted_iota(jnp.int32, (base, base), 0)
    cols_i = lax.broadcasted_iota(jnp.int32, (base, base), 1)
    spread = rows_i ^ cols_i

    def blk(i, n=1):
        return pl.ds(i * base, n * base)

    @pl.when(step == 0)
    def _():
        for i in range(blocks):
            q_i, k_i = q_ref[blk(i), :], k_ref[blk(i), :]
            s_sc[blk(i), :] = jnp.where(rows_i >= cols_i, dot_nt(q_i, k_i), 0.0)
            st_sc[blk(i), :] = jnp.where(rows_i <= cols_i, dot_nt(k_i, q_i), 0.0)
            if i > 0:
                sb_sc[blk(i), blk(0, i)] = dot_nt(q_i, k_ref[blk(0, i), :]).astype(BF)
            if i < blocks - 1:
                rest = blk(i + 1, blocks - 1 - i)
                stb_sc[blk(i), rest] = dot_nt(k_i, q_ref[rest, :]).astype(BF)
        g_sc[...] = jnp.zeros_like(g_sc)

    def factor(head):
        out = jnp.full((base, base), w_ref[head, 0], F32)
        for level in range(1, log_base + 1):
            out = jnp.where(spread >= 1 << (level - 1), w_ref[head, level], out)
        return out

    lane = lax.broadcasted_iota(jnp.int32, (base, 2 * head_dim), 1)
    left = (lane < head_dim).astype(BF)
    right = (lane >= head_dim).astype(BF)

    def stack(x):
        return jnp.concatenate([x * left, x * right], axis=0)

    mix = [[] for _ in range(blocks)]
    dv = [[] for _ in range(blocks)]
    for pair in range(heads // 2):
        span = slice(pair * 2 * head_dim, (pair + 1) * 2 * head_dim)
        f_a = factor(first_head + 2 * pair)
        f_b = factor(first_head + 2 * pair + 1)
        for i in range(blocks):
            s_i, st_i = s_sc[blk(i), :], st_sc[blk(i), :]
            v_i, c_i = v_ref[blk(i), span], c_ref[blk(i), span]
            v_stk, c_stk = stack(v_i), stack(c_i)
            w_cat = jnp.concatenate([(f_a * s_i).astype(BF), (f_b * s_i).astype(BF)], axis=1)
            mix[i].append(dot_nn(w_cat, v_stk))
            wt_cat = jnp.concatenate([(f_a * st_i).astype(BF), (f_b * st_i).astype(BF)], axis=1)
            dv[i].append(dot_nn(wt_cat, c_stk))
            raw = dot_nt(c_i, v_stk)
            g_sc[blk(i), blk(i)] += f_a * raw[:, :base] + f_b * raw[:, base:]
    for i in range(blocks):
        mix_i = jnp.concatenate(mix[i], axis=1)
        dv_i = jnp.concatenate(dv[i], axis=1)
        for k in range(log_blocks):
            other = (i >> k ^ 1) << k
            cw = cw_ref[log_base + 1 + k, :][None, :]
            there = blk(other, 1 << k)
            if i >> k & 1:
                mix_i += dot_nn(sb_sc[blk(i), there], v_ref[there, :]) * cw
                scaled = (c_ref[blk(i), :].astype(F32) * cw).astype(BF)
                g_sc[blk(i), there] += dot_nt(scaled, v_ref[there, :])
            else:
                dv_i += dot_nn(stb_sc[blk(i), there], c_ref[there, :]) * cw
        mix_ref[blk(i), :] = mix_i.astype(mix_ref.dtype)
        dv_ref[blk(i), :] = dv_i.astype(dv_ref.dtype)

    @pl.when(step == pl.num_programs(1) - 1)
    def _():
        for i in range(blocks):
            g_sc[blk(i), blk(i)] = jnp.where(rows_i >= cols_i, g_sc[blk(i), blk(i)], 0.0)
        for i in range(blocks):
            qg_ref[blk(i), :] = dot_nn(g_sc[blk(i), blk(0, i + 1)].astype(BF), k_ref[blk(0, i + 1), :])
            below = blk(i, blocks - i)
            kg_ref[blk(i), :] = dot_tn(g_sc[below, blk(i)].astype(BF), q_ref[below, :])


def intra(weights, cw_cols, values, cotangent, keys, queries, heads_local, head_dim, heads_step):
    tok, width = values.shape
    state = 128
    base = min(128, tok)
    cols = heads_step * head_dim
    steps = heads_local // heads_step
    groups = width // (heads_local * head_dim)
    col_spec = pl.BlockSpec((tok, cols), lambda g, j: (0, g * steps + j))
    row_spec = pl.BlockSpec((tok, state), lambda g, j: (0, g))
    return pl.pallas_call(
        functools.partial(intra_kernel, base=base, head_dim=head_dim),
        grid=(groups, steps),
        in_specs=[
            pl.BlockSpec(memory_space=pltpu.SMEM),
            pl.BlockSpec((cw_cols.shape[0], cols), lambda g, j: (0, g * steps + j)),
            col_spec, col_spec, row_spec, row_spec,
        ],
        out_specs=[col_spec, col_spec, row_spec, row_spec],
        out_shape=[
            jax.ShapeDtypeStruct((tok, width), BF),
            jax.ShapeDtypeStruct((tok, width), BF),
            jax.ShapeDtypeStruct((tok, groups * state), F32),
            jax.ShapeDtypeStruct((tok, groups * state), F32),
        ],
        scratch_shapes=[
            pltpu.VMEM((tok, base), F32), pltpu.VMEM((tok, base), F32),
            pltpu.VMEM((tok, tok), BF), pltpu.VMEM((tok, tok), BF),
            pltpu.VMEM((tok, tok), F32),
        ],
        cost_estimate=pl.CostEstimate(
            flops=6 * tok * tok * width, transcendentals=0, bytes_accessed=8 * tok * width
        ),
        name="intra",
    )(weights, cw_cols, values, cotangent, keys, queries)


def finish_kernel(part_ref, r_ref, flow_ref, x_ref, g_ref, o_ref, go_ref, acc):
    step = pl.program_id(1)
    flow = flow_ref[...]
    o_ref[...] = (part_ref[...].astype(F32) + dot_nt(r_ref[...], flow)).astype(o_ref.dtype)

    @pl.when(step == 0)
    def _():
        acc[...] = g_ref[...]

    acc[...] += dot_nn(x_ref[...], flow)

    @pl.when(step == pl.num_programs(1) - 1)
    def _():
        go_ref[...] = acc[...].astype(go_ref.dtype)


def finish(part, rows, flow, x, grad, cols, steps):
    tok, width = part.shape
    state = 128
    groups = width // (cols * steps)
    col_spec = pl.BlockSpec((tok, cols), lambda g, j: (0, g * steps + j))
    row_spec = pl.BlockSpec((tok, state), lambda g, j: (0, g))
    return pl.pallas_call(
        finish_kernel,
        grid=(groups, steps),
        in_specs=[
            col_spec, row_spec,
            pl.BlockSpec((cols, state), lambda g, j: (g * steps + j, 0)),
            col_spec, row_spec,
        ],
        out_specs=[col_spec, row_spec],
        out_shape=[
            jax.ShapeDtypeStruct((tok, width), BF),
            jax.ShapeDtypeStruct((tok, groups * state), BF),
        ],
        scratch_shapes=[pltpu.VMEM((tok, state), F32)],
        cost_estimate=pl.CostEstimate(
            flops=4 * tok * width * state, transcendentals=0, bytes_accessed=6 * tok * width
        ),
        name="finish",
    )(part, rows, flow, x, grad)


def per_device(
    values, group_keys, group_queries, level_table, window_index, prior_states, cotangent
):
    seq_count = lax.axis_size("seq")
    tok_rows = values.shape[0]
    heads_here = level_table.shape[0]
    head_dim = values.shape[1] // heads_here
    state_dim = group_keys.shape[2]
    group_count = group_keys.shape[1]
    prior_count = prior_states.shape[0]
    per_group = HEADS // GROUPS
    repeats = max(1, per_group // heads_here)
    local_groups = max(1, heads_here // per_group)
    heads_local = heads_here // local_groups
    log_rows = tok_rows.bit_length() - 1
    log_seq = seq_count.bit_length() - 1
    log_window = log_rows + log_seq
    width = heads_here * head_dim
    weights = level_weights(level_table)
    cw_cols = jnp.repeat(weights.T, head_dim, axis=1)
    cw_rows = jnp.repeat(weights, head_dim, axis=0)
    wide_keys = jnp.repeat(group_keys, repeats, axis=1)
    wide_queries = jnp.repeat(group_queries, repeats, axis=1)
    key_rows = lax.all_to_all(wide_keys, "head", split_axis=1, concat_axis=0, tiled=True)
    query_rows = lax.all_to_all(wide_queries, "head", split_axis=1, concat_axis=0, tiled=True)
    key_rows = key_rows.reshape(tok_rows, local_groups * state_dim)
    query_rows = query_rows.reshape(tok_rows, local_groups * state_dim)
    heads_step = min(4, heads_local)
    cols = min(8, heads_local) * head_dim
    steps = heads_local * head_dim // cols
    states = block_states(values, key_rows, cols, steps)
    adjoints = block_states(cotangent, query_rows, cols, steps)
    mix_part, dv_part, qg_part, kg_part = intra(
        weights, cw_cols, values, cotangent, key_rows, query_rows, heads_local, head_dim, heads_step
    )
    segment_index = lax.axis_index("seq")
    inflow = jnp.zeros((width, state_dim), F32)
    block_sum = states.astype(F32)
    for bit_index in range(log_seq):
        partner = partner_2(block_sum.astype(BF), "seq", bit_index).astype(F32)
        upper_half = segment_index >> bit_index & 1 == 1
        level_weight = cw_rows[:, 1 + log_rows + bit_index][:, None]
        inflow = jnp.where(upper_half, inflow + level_weight * partner, inflow)
        block_sum = block_sum + partner
    outflow = jnp.zeros((width, state_dim), F32)
    adjoint_sum = adjoints.astype(F32)
    for bit_index in range(log_seq):
        partner = partner_2(adjoint_sum.astype(BF), "seq", bit_index).astype(F32)
        lower_half = segment_index >> bit_index & 1 == 0
        level_weight = cw_rows[:, 1 + log_rows + bit_index][:, None]
        outflow = jnp.where(lower_half, outflow + level_weight * partner, outflow)
        adjoint_sum = adjoint_sum + partner
    window_bits = (window_index[0] >> jnp.arange(prior_count, dtype=jnp.int32) & 1).astype(F32)
    prior_rows = cw_rows[:, 1 + log_window : 1 + log_window + prior_count] * window_bits[None, :]
    prior_flat = prior_states.reshape(prior_count, width, state_dim)
    for level_index in range(prior_count):
        inflow = inflow + prior_rows[:, level_index][:, None] * prior_flat[level_index].astype(F32)
    inflow_cast = inflow.astype(BF)
    outflow_cast = outflow.astype(BF)
    grad_prior = (prior_rows.T[:, :, None] * adjoint_sum[None]).reshape(prior_states.shape)
    mixer_out, query_part = finish(mix_part, query_rows, inflow_cast, cotangent, qg_part, cols, steps)
    grad_values, key_part = finish(dv_part, key_rows, outflow_cast, values, kg_part, cols, steps)

    def back(part):
        part = part.reshape(tok_rows, local_groups, state_dim)
        part = lax.all_to_all(part, "head", split_axis=0, concat_axis=1, tiled=True).astype(F32)
        return part.reshape(part.shape[0], group_count, repeats, state_dim).sum(axis=2)

    return (mixer_out, grad_values, back(key_part), back(query_part), grad_prior)


def solution(mesh):
    placed = (
        P("seq", "head"),
        P(("seq", "head"), None, None),
        P(("seq", "head"), None, None),
        P("head", None),
        P(),
        P(None, "head", None, None),
        P("seq", "head"),
    )
    return jax.shard_map(
        per_device,
        mesh=mesh,
        in_specs=placed,
        out_specs=(
            P("seq", "head"),
            P("seq", "head"),
            P(("seq", "head"), None, None),
            P(("seq", "head"), None, None),
            P(None, "head", None, None),
        ),
        check_vma=False,
    )
```

```python
import functools

import jax
import jax.numpy as jnp
from jax import lax
from jax.experimental import pallas as pl
from jax.experimental.pallas import tpu as pltpu
from jax.sharding import PartitionSpec as P


HEADS = 128
GROUPS = 8
BF = jnp.bfloat16
F32 = jnp.float32
SMEM = pl.BlockSpec(memory_space=pltpu.SMEM)
VMEM = pl.BlockSpec(memory_space=pltpu.VMEM)
PARAMS = pltpu.CompilerParams(vmem_limit_bytes=24 << 20)


def near_core(array):
    return pltpu.with_memory_space_constraint(array, pltpu.VMEM)


def swap_with(array, axis, mask):
    return lax.ppermute(array, axis, [(i, i ^ mask) for i in range(lax.axis_size(axis))])


def dot_nn(a, b):
    return lax.dot_general(a, b, (((1,), (0,)), ((), ())), preferred_element_type=F32)


def dot_nt(a, b):
    return lax.dot_general(a, b, (((1,), (1,)), ((), ())), preferred_element_type=F32)


def dot_tn(a, b):
    return lax.dot_general(a, b, (((0,), (0,)), ((), ())), preferred_element_type=F32)


def shaped(shape, dtype):
    return jax.ShapeDtypeStruct(shape, dtype)


def cost(flops, bytes_accessed):
    return pl.CostEstimate(flops=flops, transcendentals=0, bytes_accessed=bytes_accessed)


def weight(table_ref, head, level):
    return table_ref[head, level].astype(F32) * 2.0 ** (-max(level - 1, 0) / 2)


def log2(number):
    return number.bit_length() - 1


def prep_kernel(*refs, pieces):
    x_refs, outs, scratch = refs[:2], refs[2:-1], refs[-1]
    here = lax.axis_index("head")
    for n, x_ref in enumerate(x_refs):
        scratch[...] = jnp.swapaxes(x_ref[...].astype(F32), 0, 1)
        for r, out in enumerate(outs[n * pieces : (n + 1) * pieces]):
            take = out.shape[0]
            out[...] = scratch[pl.ds((here ^ r) * take, take)].astype(out.dtype)


def prep(keys, queries, pieces):
    rows, groups, state = keys.shape
    out = pl.pallas_call(
        functools.partial(prep_kernel, pieces=pieces),
        in_specs=[VMEM] * 2,
        out_specs=[VMEM] * (2 * pieces),
        out_shape=[pltpu.VMEM((groups // pieces, rows, state), BF)] * (2 * pieces),
        scratch_shapes=[pltpu.VMEM((groups, rows, state), F32)],
        compiler_params=PARAMS,
        cost_estimate=cost(10**6, 8 * keys.size),
        name="prep",
    )(keys, queries)
    return out[:pieces], out[pieces:]


def states_kernel(x_ref, *refs):
    parts, (o_ref, rows_ref) = refs[:-2], refs[-2:]
    if len(parts) == 1:
        rows_ref[...] = parts[0][...]
    else:
        here = lax.axis_index("head")
        size = parts[0].shape[1]
        for r, part in enumerate(parts):
            rows_ref[:, pl.ds(pl.multiple_of((here ^ r) * size, size), size), :] = part[...]
    groups = rows_ref.shape[0]
    width = x_ref.shape[1] // groups
    for g in range(groups):
        span = slice(g * width, (g + 1) * width)
        o_ref[span, :] = dot_tn(rows_ref[g], x_ref[:, span]).T.astype(o_ref.dtype)


def block_states(x, parts):
    tok, width = x.shape
    lg, _, state = parts[0].shape
    return pl.pallas_call(
        states_kernel,
        in_specs=[VMEM] * (1 + len(parts)),
        out_specs=[VMEM] * 2,
        out_shape=[pltpu.VMEM((width, state), BF), pltpu.VMEM((lg, tok, state), BF)],
        compiler_params=PARAMS,
        cost_estimate=cost(2 * tok * width * state, 2 * tok * width),
        name="states",
    )(x, *[near_core(part) for part in parts])


def spread_grid(base):
    rows = lax.broadcasted_iota(jnp.int32, (base, base), 0)
    cols = lax.broadcasted_iota(jnp.int32, (base, base), 1)
    return rows, cols, rows ^ cols


def factor_of(table_ref, head, spread, base):
    out = jnp.full((base, base), weight(table_ref, head, 0), F32)
    for level in range(1, log2(base) + 1):
        out = jnp.where(spread >= 1 << (level - 1), weight(table_ref, head, level), out)
    return out


def sides(base, head_dim):
    lane = lax.broadcasted_iota(jnp.int32, (base, 2 * head_dim), 1)
    return lane < head_dim, (lane < head_dim).astype(BF), (lane >= head_dim).astype(BF)


def blk(i, base, n=1):
    return pl.ds(i * base, n * base)


def pair_weights(table_ref, first_head, pairs, level, is_left):
    rows = [
        jnp.where(
            is_left,
            weight(table_ref, first_head + 2 * p, level),
            weight(table_ref, first_head + 2 * p + 1, level),
        )
        for p in range(pairs)
    ]
    return jnp.concatenate(rows, axis=1)


def gram_kernel(table_ref, v_ref, c_ref, g_ref, g_sc, *, base, head_dim, group, cols):
    tok = v_ref.shape[0]
    blocks = tok // base
    heads = cols // head_dim
    step = pl.program_id(0)
    at = group * pl.num_programs(0) + step
    first_head = at * heads
    first_col = pl.multiple_of(at * cols, cols)
    rows_i, cols_i, spread = spread_grid(base)
    is_left, left, right = sides(base, head_dim)

    @pl.when(step == 0)
    def _():
        g_sc[...] = jnp.zeros_like(g_sc)

    for pair in range(heads // 2):
        span = pl.ds(first_col + pair * 2 * head_dim, 2 * head_dim)
        f_a = factor_of(table_ref, first_head + 2 * pair, spread, base)
        f_b = factor_of(table_ref, first_head + 2 * pair + 1, spread, base)
        for i in range(blocks):
            v_i, c_i = v_ref[blk(i, base), span], c_ref[blk(i, base), span]
            raw = dot_nt(c_i, jnp.concatenate([v_i * left, v_i * right], axis=0))
            g_sc[blk(i, base), blk(i, base)] += f_a * raw[:, :base] + f_b * raw[:, base:]
    span = pl.ds(first_col, cols)
    for k in range(log2(blocks)):
        cw = pair_weights(table_ref, first_head, heads // 2, log2(base) + 1 + k, is_left[:1])
        for i in range(blocks):
            if i >> k & 1:
                there = blk((i >> k ^ 1) << k, base, 1 << k)
                scaled = (c_ref[blk(i, base), span].astype(F32) * cw).astype(BF)
                g_sc[blk(i, base), there] += dot_nt(scaled, v_ref[there, span])

    @pl.when(step == pl.num_programs(0) - 1)
    def _():
        for i in range(blocks):
            here = blk(i, base)
            g_sc[here, here] = jnp.where(rows_i >= cols_i, g_sc[here, here], 0.0)
        g_ref[...] = g_sc[...].astype(BF)


def gram(table, values, cotangent, group, groups, head_dim, cols):
    tok, width = values.shape
    base = min(128, tok)
    return pl.pallas_call(
        functools.partial(gram_kernel, base=base, head_dim=head_dim, group=group, cols=cols),
        grid=(width // groups // cols,),
        in_specs=[SMEM, VMEM, VMEM],
        out_specs=VMEM,
        out_shape=pltpu.VMEM((tok, tok), BF),
        scratch_shapes=[pltpu.VMEM((tok, tok), F32)],
        compiler_params=PARAMS,
        cost_estimate=cost(2 * tok * tok * width // groups, 4 * tok * width // groups),
        name="gram",
    )(table, values, cotangent)


def intra_kernel(table_ref, v_ref, c_ref, kg_rows, qg_rows, g_ref, *refs, base, head_dim, group, cols):
    mix_ref, dv_ref, qg_ref, kg_ref, s_sc, st_sc, sb_sc, stb_sc = refs[-8:]
    k_ref, q_ref = kg_rows.at[group], qg_rows.at[group]
    tok = v_ref.shape[0]
    blocks = tok // base
    heads = cols // head_dim
    step = pl.program_id(0)
    at = group * pl.num_programs(0) + step
    first_head = at * heads
    first_col = pl.multiple_of(at * cols, cols)
    rows_i, cols_i, spread = spread_grid(base)
    is_left, left, right = sides(base, head_dim)

    @pl.when(step == 0)
    def _():
        for i in range(blocks):
            here = blk(i, base)
            q_i, k_i = q_ref[here, :], k_ref[here, :]
            s_sc[here, :] = jnp.where(rows_i >= cols_i, dot_nt(q_i, k_i), 0.0)
            st_sc[here, :] = jnp.where(rows_i <= cols_i, dot_nt(k_i, q_i), 0.0)
            above = blk(0, base, i)
            rest = blk(i + 1, base, blocks - 1 - i)
            if i > 0:
                sb_sc[here, above] = dot_nt(q_i, k_ref[above, :]).astype(BF)
            if i < blocks - 1:
                stb_sc[here, rest] = dot_nt(k_i, q_ref[rest, :]).astype(BF)
            until = blk(0, base, i + 1)
            below = blk(i, base, blocks - i)
            qg_ref[here, :] = dot_nn(g_ref[here, until], k_ref[until, :])
            kg_ref[here, :] = dot_tn(g_ref[below, here], q_ref[below, :])

    mix = [[] for _ in range(blocks)]
    dv = [[] for _ in range(blocks)]
    for pair in range(heads // 2):
        span = pl.ds(first_col + pair * 2 * head_dim, 2 * head_dim)
        f_a = factor_of(table_ref, first_head + 2 * pair, spread, base)
        f_b = factor_of(table_ref, first_head + 2 * pair + 1, spread, base)
        for i in range(blocks):
            here = blk(i, base)
            for f_ref, x_ref, out in ((s_sc, v_ref, mix), (st_sc, c_ref, dv)):
                s_i, x_i = f_ref[here, :], x_ref[here, span]
                w_cat = jnp.concatenate([(f_a * s_i).astype(BF), (f_b * s_i).astype(BF)], axis=1)
                stacked = jnp.concatenate([x_i * left, x_i * right], axis=0)
                out[i].append(dot_nn(w_cat, stacked))
    scales = [
        pair_weights(table_ref, first_head, heads // 2, log2(base) + 1 + k, is_left[:1])
        for k in range(log2(blocks))
    ]
    span = pl.ds(first_col, cols)
    for i in range(blocks):
        here = blk(i, base)
        mix_i = jnp.concatenate(mix[i], axis=1)
        dv_i = jnp.concatenate(dv[i], axis=1)
        for k, cw in enumerate(scales):
            there = blk((i >> k ^ 1) << k, base, 1 << k)
            if i >> k & 1:
                mix_i += dot_nn(sb_sc[here, there], v_ref[there, span]) * cw
            else:
                dv_i += dot_nn(stb_sc[here, there], c_ref[there, span]) * cw
        mix_ref[here, span] = mix_i.astype(mix_ref.dtype)
        dv_ref[here, span] = dv_i.astype(dv_ref.dtype)


def intra(table, values, cotangent, keys, queries, grams, before, group, head_dim, cols):
    tok, width = values.shape
    groups, _, state = keys.shape
    base = min(128, tok)
    return pl.pallas_call(
        functools.partial(intra_kernel, base=base, head_dim=head_dim, group=group, cols=cols),
        grid=(width // groups // cols,),
        in_specs=[SMEM] + [VMEM] * (5 + len(before)),
        out_specs=[VMEM] * 4,
        out_shape=[pltpu.VMEM((tok, width), BF)] * 2 + [pltpu.VMEM((tok, state), F32)] * 2,
        input_output_aliases={6 + n: n for n in range(len(before))},
        scratch_shapes=[pltpu.VMEM((tok, base), F32)] * 2 + [pltpu.VMEM((tok, tok), BF)] * 2,
        compiler_params=PARAMS,
        cost_estimate=cost(4 * tok * tok * width // groups, 8 * tok * width // groups),
        name="intra",
    )(table, values, cotangent, keys, queries, grams, *before)


def near_kernel(table_ref, window_ref, p_ref, *refs, level, gate, head_dim, prior_level):
    o_ref = refs[-1]
    priors = refs[0] if len(refs) > 1 else None
    heads = o_ref.shape[0] // head_dim
    on = (lax.axis_index("seq") & 1 == gate).astype(F32)
    for h in range(heads):
        rows = blk(h, head_dim)
        out = p_ref[rows, :].astype(F32) * (weight(table_ref, h, level) * on)
        if priors is not None:
            for k in range(priors.shape[0]):
                bit = (window_ref[0] >> k & 1).astype(F32)
                out += priors[k, rows, :].astype(F32) * (weight(table_ref, h, prior_level + k) * bit)
        o_ref[rows, :] = out


def near(table, window, partner, priors, level, gate, head_dim, prior_level):
    width, state = partner.shape
    ins = [near_core(x) for x in (partner, priors) if x is not None]
    return pl.pallas_call(
        functools.partial(
            near_kernel, level=level, gate=gate, head_dim=head_dim, prior_level=prior_level
        ),
        in_specs=[SMEM, SMEM] + [VMEM] * len(ins),
        out_specs=VMEM,
        out_shape=pltpu.VMEM((width, state), F32),
        compiler_params=PARAMS,
        cost_estimate=cost(10 * width * state, 8 * width * state),
        name="near",
    )(table, window, *ins)


def combine_kernel(a_ref, b_ref, o_ref):
    half = o_ref.shape[0]
    rows = pl.ds(0, half)
    if a_ref.shape[0] > half:
        rows = pl.ds(pl.multiple_of((lax.axis_index("seq") & 1) * half, half), half)
    total = a_ref[rows, :].astype(F32) + b_ref[rows, :].astype(F32)
    o_ref[...] = total.astype(o_ref.dtype)


def combine(a, b, half):
    return pl.pallas_call(
        combine_kernel,
        in_specs=[VMEM] * 2,
        out_specs=VMEM,
        out_shape=pltpu.VMEM((half, a.shape[1]), BF),
        compiler_params=PARAMS,
        cost_estimate=cost(a.size, 4 * a.size),
        name="combine",
    )(near_core(a), near_core(b))


def far_kernel(table_ref, *refs, level, gate, head_dim, with_total):
    o_ref = refs[-1]
    partners = refs[:-2] if with_total else refs[:-1]
    half = partners[0].shape[0]
    heads = half // head_dim
    seq = lax.axis_index("seq")
    first = (seq & 1) * heads
    ons = [(seq >> (k + 1) & 1 == gate).astype(F32) for k in range(len(partners))]
    for h in range(heads):
        rows = blk(h, head_dim)
        out = None
        for k, p_ref in enumerate(partners):
            term = p_ref[rows, :].astype(F32) * (
                weight(table_ref, first + h, level + k) * ons[k]
            )
            out = term if out is None else out + term
        o_ref[rows, :] = out.astype(o_ref.dtype)
    if with_total:
        total = refs[-2][...].astype(F32) + partners[-1][...].astype(F32)
        o_ref[pl.ds(half, half), :] = total.astype(o_ref.dtype)


def far(table, partners, before, level, gate, head_dim):
    half, state = partners[0].shape
    extra = [] if before is None else [before]
    return pl.pallas_call(
        functools.partial(
            far_kernel, level=level, gate=gate, head_dim=head_dim, with_total=bool(extra)
        ),
        in_specs=[SMEM] + [VMEM] * (len(partners) + len(extra)),
        out_specs=VMEM,
        out_shape=pltpu.VMEM((half * (1 + len(extra)), state), BF),
        compiler_params=PARAMS,
        cost_estimate=cost(10 * half * state, 8 * half * state),
        name="far",
    )(table, *[near_core(x) for x in partners + extra])


def finish_kernel(
    part_ref, r_ref, near_ref, mine_ref, other_ref, x_ref, *refs, pieces, halves, cols
):
    groups = r_ref.shape[0]
    g_refs, o_ref, outs, acc = refs[:groups], refs[groups], refs[groups + 1 : -1], refs[-1]
    group, step = pl.program_id(0), pl.program_id(1)
    at = group * pl.num_programs(1) + step
    is_mine = at // halves == lax.axis_index("seq") & 1
    span = pl.ds(pl.multiple_of(at * cols, cols), cols)
    half = pl.ds(pl.multiple_of(at % halves * cols, cols), cols)
    flow = near_ref[span, :] + jnp.where(is_mine, mine_ref[half, :], other_ref[half, :]).astype(F32)
    flow = flow.astype(BF)
    o_ref[...] = (part_ref[:, span].astype(F32) + dot_nt(r_ref[group], flow)).astype(o_ref.dtype)
    for g in range(groups):

        @pl.when((step == 0) & (group == g))
        def _():
            acc[...] = g_refs[g][...]

    acc[...] += dot_nn(x_ref[:, span], flow)

    @pl.when(step == pl.num_programs(1) - 1)
    def _():
        if pieces == 1:
            outs[0][group] = acc[...].astype(BF)
        else:
            here = lax.axis_index("head")
            size = outs[0].shape[1]
            for r, out in enumerate(outs):
                rows = pl.ds(pl.multiple_of((here ^ r) * size, size), size)
                out[group] = acc[rows, :].astype(BF)


def finish(part, rows, near_flow, mine, other, x, grads, cols, pieces):
    tok, width = part.shape
    groups, _, state = rows.shape
    steps = width // groups // cols
    piece = (groups, tok // pieces, state)
    return pl.pallas_call(
        functools.partial(finish_kernel, pieces=pieces, halves=width // cols // 2, cols=cols),
        grid=(groups, steps),
        in_specs=[VMEM] * (6 + groups),
        out_specs=[pl.BlockSpec((tok, cols), lambda g, j: (0, g * steps + j))] + [VMEM] * pieces,
        out_shape=[shaped((tok, width), BF)] + [pltpu.VMEM(piece, BF)] * pieces,
        scratch_shapes=[pltpu.VMEM((tok, state), F32)],
        compiler_params=PARAMS,
        cost_estimate=cost(4 * tok * width * state, 6 * tok * width),
        name="finish",
    )(part, rows, near_flow, near_core(mine), near_core(other), x, *grads)


def gather_kernel(*refs):
    parts, o_ref, scratch = refs[:-2], refs[-2], refs[-1]
    here = lax.axis_index("head")
    take = parts[0].shape[0]
    for r, part in enumerate(parts):
        scratch[pl.ds((here ^ r) * take, take)] = part[...].astype(F32)
    o_ref[...] = jnp.swapaxes(scratch[...], 0, 1)


def gather(parts):
    take, rows, state = parts[0].shape
    groups = take * len(parts)
    return pl.pallas_call(
        gather_kernel,
        in_specs=[VMEM] * len(parts),
        out_specs=pl.BlockSpec((rows, groups, state), lambda: (0, 0, 0)),
        out_shape=shaped((rows, groups, state), F32),
        scratch_shapes=[pltpu.VMEM((groups, rows, state), F32)],
        compiler_params=PARAMS,
        cost_estimate=cost(10**6, 6 * groups * rows * state),
        name="gather",
    )(*[near_core(part) for part in parts])


def prior_kernel(table_ref, window_ref, mine_ref, other_ref, o_ref, *, head_dim, level, halves):
    at = pl.program_id(0)
    size = o_ref.shape[1]
    heads = size // head_dim
    is_mine = at // halves == lax.axis_index("seq") & 1
    rows = pl.ds(pl.multiple_of((halves + at % halves) * size, size), size)
    total = jnp.where(is_mine, mine_ref[rows, :], other_ref[rows, :]).astype(F32)
    for h in range(heads):
        rows = slice(h * head_dim, (h + 1) * head_dim)
        for k in range(o_ref.shape[0]):
            bit = (window_ref[0] >> k & 1).astype(F32)
            o_ref[k, rows, :] = total[rows] * (weight(table_ref, at * heads + h, level + k) * bit)


def prior_grad(table, window, mine, other, count, level, head_dim, steps):
    half = mine.shape[0] // 2
    state = mine.shape[1]
    halves = steps // 2
    rows = half // halves
    return pl.pallas_call(
        functools.partial(prior_kernel, head_dim=head_dim, level=level, halves=halves),
        grid=(steps,),
        in_specs=[SMEM, SMEM, VMEM, VMEM],
        out_specs=pl.BlockSpec((count, rows, state), lambda i: (0, i, 0)),
        out_shape=shaped((count, 2 * half, state), F32),
        compiler_params=PARAMS,
        cost_estimate=cost(2 * count * half * state, 8 * count * half * state),
        name="prior_grad",
    )(table, window, near_core(mine), near_core(other))


def mixer(
    values, group_keys, group_queries, level_table, window_index, prior_states, cotangent
):
    seq_count = lax.axis_size("seq")
    head_count = lax.axis_size("head")
    tok_rows = values.shape[0]
    heads_here = level_table.shape[0]
    head_dim = values.shape[1] // heads_here
    state_dim = group_keys.shape[2]
    group_count = group_keys.shape[1]
    prior_count = prior_states.shape[0]
    per_group = HEADS // GROUPS
    repeats = max(1, per_group // heads_here)
    local_groups = max(1, heads_here // per_group)
    heads_local = heads_here // local_groups
    log_rows = log2(tok_rows)
    log_seq = log2(seq_count)
    log_window = log_rows + log_seq
    width = heads_here * head_dim
    half = width // 2
    pieces = head_count if head_count <= 4 and repeats == 1 else 1
    cols_in = min(4, heads_local) * head_dim
    cols = min(8, heads_here // 2) * head_dim

    def scattered(own, *sent):
        out = [own]
        for r, part in enumerate(sent):
            out.append(swap_with(part, "head", r + 1))
        return out

    def rows_of(x):
        wide = jnp.repeat(x, repeats, axis=1).swapaxes(0, 1)
        wide = wide.reshape(head_count, local_groups, -1, state_dim)
        wide = lax.all_to_all(wide, "head", split_axis=0, concat_axis=0)
        return [wide.swapaxes(0, 1).reshape(local_groups, tok_rows, state_dim)]

    if pieces == 1:
        key_parts, query_parts = rows_of(group_keys), rows_of(group_queries)
    else:
        key_parts, query_parts = prep(group_keys, group_queries, pieces)
        key_parts = scattered(*key_parts)
        query_parts = scattered(*query_parts)
    values, cotangent = near_core(values), near_core(cotangent)
    grams = []
    for g in range(local_groups):
        grams.append(
            gram(level_table, values, cotangent, g, local_groups, head_dim, cols_in)
        )

    def exchange(own, gate, priors):
        partner = swap_with(own, "seq", 1)
        near_flow = near(
            level_table, window_index, partner, priors, 1 + log_rows, gate, head_dim,
            1 + log_window,
        )
        total = combine(own, partner, half)
        partners = []
        for bit in range(1, log_seq):
            partners.append(swap_with(total, "seq", 1 << bit))
            if bit < log_seq - 1:
                total = combine(total, partners[-1], half)
        before = None if priors is not None else total
        mine = far(level_table, partners, before, 2 + log_rows, gate, head_dim)
        other = swap_with(mine, "seq", 1)
        return near_flow, mine, other

    states, key_rows = block_states(values, key_parts)
    priors = prior_states.reshape(prior_count, width, state_dim)
    in_near, in_mine, in_other = exchange(states, 1, priors)
    adjoints, query_rows = block_states(cotangent, query_parts)
    out_near, out_mine, out_other = exchange(adjoints, 0, None)
    parts, query_grads, key_grads = [], [], []
    for g in range(local_groups):
        *parts, query_grad, key_grad = intra(
            level_table, values, cotangent, key_rows, query_rows, grams[g], parts, g,
            head_dim, cols_in,
        )
        query_grads.append(query_grad)
        key_grads.append(key_grad)
    mix_part, dv_part = parts

    def back(parts):
        if pieces == 1:
            part = parts[0].reshape(local_groups, head_count, -1, state_dim).swapaxes(0, 1)
            part = lax.all_to_all(part, "head", split_axis=0, concat_axis=0).astype(F32)
            part = part.reshape(group_count, repeats, -1, state_dim).sum(axis=1)
            return part.swapaxes(0, 1)
        parts = scattered(*parts)
        return gather(parts)

    mixer_out, *query_parts = finish(
        mix_part, query_rows, in_near, in_mine, in_other, cotangent, query_grads, cols, pieces
    )
    grad_queries = back(query_parts)
    grad_values, *key_parts = finish(
        dv_part, key_rows, out_near, out_mine, out_other, values, key_grads, cols, pieces
    )
    grad_keys = back(key_parts)
    grad_prior = prior_grad(
        level_table, window_index, out_mine, out_other, prior_count, 1 + log_window, head_dim,
        width // cols,
    )
    return (mixer_out, grad_values, grad_keys, grad_queries, grad_prior.reshape(prior_states.shape))


def solution(mesh):
    placed = (
        P("seq", "head"),
        P(("seq", "head"), None, None),
        P(("seq", "head"), None, None),
        P("head", None),
        P(),
        P(None, "head", None, None),
        P("seq", "head"),
    )
    return jax.shard_map(
        mixer,
        mesh=mesh,
        in_specs=placed,
        out_specs=(
            P("seq", "head"),
            P("seq", "head"),
            P(("seq", "head"), None, None),
            P(("seq", "head"), None, None),
            P(None, "head", None, None),
        ),
        check_vma=False,
    )
```

```python
import functools

import jax
import jax.numpy as jnp
from jax import lax
from jax.experimental import pallas as pl
from jax.experimental.pallas import tpu as pltpu
from jax.sharding import PartitionSpec as P


HEADS = 128
GROUPS = 8
BF = jnp.bfloat16
F32 = jnp.float32
SMEM = pl.BlockSpec(memory_space=pltpu.SMEM)
VMEM = pl.BlockSpec(memory_space=pltpu.VMEM)
HBM = pl.BlockSpec(memory_space=pltpu.HBM)
PARAMS = pltpu.CompilerParams(vmem_limit_bytes=24 << 20)


def near_core(array):
    return pltpu.with_memory_space_constraint(array, pltpu.VMEM)


def far_off(array):
    return pltpu.with_memory_space_constraint(array, pltpu.HBM)


def swap_with(array, axis, mask):
    return lax.ppermute(array, axis, [(i, i ^ mask) for i in range(lax.axis_size(axis))])


def dot_nn(a, b):
    return lax.dot_general(a, b, (((1,), (0,)), ((), ())), preferred_element_type=F32)


def dot_nt(a, b):
    return lax.dot_general(a, b, (((1,), (1,)), ((), ())), preferred_element_type=F32)


def dot_tn(a, b):
    return lax.dot_general(a, b, (((0,), (0,)), ((), ())), preferred_element_type=F32)


def shaped(shape, dtype):
    return jax.ShapeDtypeStruct(shape, dtype)


def cost(flops, bytes_accessed):
    return pl.CostEstimate(flops=flops, transcendentals=0, bytes_accessed=bytes_accessed)


def weight(table_ref, head, level):
    return table_ref[level, head].astype(F32) * 2.0 ** (-max(level - 1, 0) / 2)


def log2(number):
    return number.bit_length() - 1


def prep_kernel(*refs, pieces):
    x_refs, big, refs = refs[:2], refs[2:4], refs[4:]
    outs, big_outs = refs[: 2 * pieces], refs[2 * pieces : 2 * pieces + 2]
    raw, scratch, sems = refs[2 * pieces + 2 :]
    here = lax.axis_index("head")
    copies = [pltpu.make_async_copy(x, raw.at[n], sems.at[n]) for n, x in enumerate(x_refs)]
    copies += [
        pltpu.make_async_copy(x, out, sems.at[2 + n])
        for n, (x, out) in enumerate(zip(big, big_outs))
    ]
    for copy in copies:
        copy.start()
    for n in range(2):
        copies[n].wait()
        scratch[...] = jnp.swapaxes(raw[n].astype(F32), 0, 1)
        for r, out in enumerate(outs[n * pieces : (n + 1) * pieces]):
            take = out.shape[0]
            out[...] = scratch[pl.ds((here ^ r) * take, take)].astype(out.dtype)
    copies[2].wait()
    copies[3].wait()


def prep(keys, queries, values, cotangent, pieces):
    rows, groups, state = keys.shape
    out = pl.pallas_call(
        functools.partial(prep_kernel, pieces=pieces),
        in_specs=[HBM] * 4,
        out_specs=[VMEM] * (2 * pieces + 2),
        out_shape=[pltpu.VMEM((groups // pieces, rows, state), BF)] * (2 * pieces)
        + [pltpu.VMEM(values.shape, BF)] * 2,
        scratch_shapes=[
            pltpu.VMEM((2,) + keys.shape, BF),
            pltpu.VMEM((groups, rows, state), F32),
            pltpu.SemaphoreType.DMA((4,)),
        ],
        compiler_params=PARAMS,
        cost_estimate=cost(10**6, 8 * keys.size),
        name="prep",
    )(*[far_off(x) for x in (keys, queries, values, cotangent)])
    return out[:pieces], out[pieces : 2 * pieces], out[-2], out[-1]


def states_kernel(x_ref, *refs):
    parts, (o_ref, rows_ref) = refs[:-2], refs[-2:]
    if len(parts) == 1:
        rows_ref[...] = parts[0][...]
    else:
        here = lax.axis_index("head")
        size = parts[0].shape[1]
        for r, part in enumerate(parts):
            rows_ref[:, pl.ds(pl.multiple_of((here ^ r) * size, size), size), :] = part[...]
    groups = rows_ref.shape[0]
    width = x_ref.shape[1] // groups
    for g in range(groups):
        span = slice(g * width, (g + 1) * width)
        o_ref[span, :] = dot_tn(rows_ref[g], x_ref[:, span]).T.astype(o_ref.dtype)


def block_states(x, parts):
    tok, width = x.shape
    lg, _, state = parts[0].shape
    return pl.pallas_call(
        states_kernel,
        in_specs=[VMEM] * (1 + len(parts)),
        out_specs=[VMEM] * 2,
        out_shape=[pltpu.VMEM((width, state), BF), pltpu.VMEM((lg, tok, state), BF)],
        compiler_params=PARAMS,
        cost_estimate=cost(2 * tok * width * state, 2 * tok * width),
        name="states",
    )(x, *[near_core(part) for part in parts])


def spread_grid(base):
    rows = lax.broadcasted_iota(jnp.int32, (base, base), 0)
    cols = lax.broadcasted_iota(jnp.int32, (base, base), 1)
    return rows, cols, rows ^ cols


def factor_of(table_ref, head, spread, base):
    out = jnp.full((base, base), weight(table_ref, head, 0), F32)
    for level in range(1, log2(base) + 1):
        out = jnp.where(spread >= 1 << (level - 1), weight(table_ref, head, level), out)
    return out


def sides(base, head_dim):
    lane = lax.broadcasted_iota(jnp.int32, (base, 2 * head_dim), 1)
    return lane < head_dim, (lane < head_dim).astype(BF), (lane >= head_dim).astype(BF)


def blk(i, base, n=1):
    return pl.ds(i * base, n * base)


def pair_weights(table_ref, first_head, pairs, level, is_left):
    rows = [
        jnp.where(
            is_left,
            weight(table_ref, first_head + 2 * p, level),
            weight(table_ref, first_head + 2 * p + 1, level),
        )
        for p in range(pairs)
    ]
    return jnp.concatenate(rows, axis=1)


def gram_kernel(table_ref, v_ref, c_ref, g_ref, g_sc, *, base, head_dim, group, cols):
    tok = v_ref.shape[0]
    blocks = tok // base
    heads = cols // head_dim
    step = pl.program_id(0)
    at = group * pl.num_programs(0) + step
    first_head = at * heads
    first_col = pl.multiple_of(at * cols, cols)
    rows_i, cols_i, spread = spread_grid(base)
    is_left, left, right = sides(base, head_dim)

    @pl.when(step == 0)
    def _():
        g_sc[...] = jnp.zeros_like(g_sc)

    for pair in range(heads // 2):
        span = pl.ds(first_col + pair * 2 * head_dim, 2 * head_dim)
        f_a = factor_of(table_ref, first_head + 2 * pair, spread, base)
        f_b = factor_of(table_ref, first_head + 2 * pair + 1, spread, base)
        for i in range(blocks):
            v_i, c_i = v_ref[blk(i, base), span], c_ref[blk(i, base), span]
            raw = dot_nt(c_i, jnp.concatenate([v_i * left, v_i * right], axis=0))
            g_sc[blk(i, base), blk(i, base)] += f_a * raw[:, :base] + f_b * raw[:, base:]
    span = pl.ds(first_col, cols)
    for k in range(log2(blocks)):
        cw = pair_weights(table_ref, first_head, heads // 2, log2(base) + 1 + k, is_left[:1])
        for i in range(blocks):
            if i >> k & 1:
                there = blk((i >> k ^ 1) << k, base, 1 << k)
                scaled = (c_ref[blk(i, base), span].astype(F32) * cw).astype(BF)
                g_sc[blk(i, base), there] += dot_nt(scaled, v_ref[there, span])

    @pl.when(step == pl.num_programs(0) - 1)
    def _():
        for i in range(blocks):
            here = blk(i, base)
            g_sc[here, here] = jnp.where(rows_i >= cols_i, g_sc[here, here], 0.0)
        g_ref[...] = g_sc[...].astype(BF)


def gram(table, values, cotangent, group, groups, head_dim, cols):
    tok, width = values.shape
    base = min(128, tok)
    return pl.pallas_call(
        functools.partial(gram_kernel, base=base, head_dim=head_dim, group=group, cols=cols),
        grid=(width // groups // cols,),
        in_specs=[SMEM, VMEM, VMEM],
        out_specs=VMEM,
        out_shape=pltpu.VMEM((tok, tok), BF),
        scratch_shapes=[pltpu.VMEM((tok, tok), F32)],
        compiler_params=PARAMS,
        cost_estimate=cost(2 * tok * tok * width // groups, 4 * tok * width // groups),
        name="gram",
    )(table, values, cotangent)


def intra_kernel(table_ref, v_ref, c_ref, kg_rows, qg_rows, g_ref, *refs, base, head_dim, group, cols):
    mix_ref, dv_ref, qg_ref, kg_ref, s_sc, st_sc, sb_sc, stb_sc = refs[-8:]
    k_ref, q_ref = kg_rows.at[group], qg_rows.at[group]
    tok = v_ref.shape[0]
    blocks = tok // base
    heads = cols // head_dim
    step = pl.program_id(0)
    at = group * pl.num_programs(0) + step
    first_head = at * heads
    first_col = pl.multiple_of(at * cols, cols)
    rows_i, cols_i, spread = spread_grid(base)
    is_left, left, right = sides(base, head_dim)

    @pl.when(step == 0)
    def _():
        for i in range(blocks):
            here = blk(i, base)
            q_i, k_i = q_ref[here, :], k_ref[here, :]
            s_sc[here, :] = jnp.where(rows_i >= cols_i, dot_nt(q_i, k_i), 0.0)
            st_sc[here, :] = jnp.where(rows_i <= cols_i, dot_nt(k_i, q_i), 0.0)
            above = blk(0, base, i)
            rest = blk(i + 1, base, blocks - 1 - i)
            if i > 0:
                sb_sc[here, above] = dot_nt(q_i, k_ref[above, :]).astype(BF)
            if i < blocks - 1:
                stb_sc[here, rest] = dot_nt(k_i, q_ref[rest, :]).astype(BF)
            until = blk(0, base, i + 1)
            below = blk(i, base, blocks - i)
            qg_ref[here, :] = dot_nn(g_ref[here, until], k_ref[until, :])
            kg_ref[here, :] = dot_tn(g_ref[below, here], q_ref[below, :])

    mix = [[] for _ in range(blocks)]
    dv = [[] for _ in range(blocks)]
    for pair in range(heads // 2):
        span = pl.ds(first_col + pair * 2 * head_dim, 2 * head_dim)
        f_a = factor_of(table_ref, first_head + 2 * pair, spread, base)
        f_b = factor_of(table_ref, first_head + 2 * pair + 1, spread, base)
        for i in range(blocks):
            here = blk(i, base)
            for f_ref, x_ref, out in ((s_sc, v_ref, mix), (st_sc, c_ref, dv)):
                s_i, x_i = f_ref[here, :], x_ref[here, span]
                w_cat = jnp.concatenate([(f_a * s_i).astype(BF), (f_b * s_i).astype(BF)], axis=1)
                stacked = jnp.concatenate([x_i * left, x_i * right], axis=0)
                out[i].append(dot_nn(w_cat, stacked))
    scales = [
        pair_weights(table_ref, first_head, heads // 2, log2(base) + 1 + k, is_left[:1])
        for k in range(log2(blocks))
    ]
    span = pl.ds(first_col, cols)
    for i in range(blocks):
        here = blk(i, base)
        mix_i = jnp.concatenate(mix[i], axis=1)
        dv_i = jnp.concatenate(dv[i], axis=1)
        for k, cw in enumerate(scales):
            there = blk((i >> k ^ 1) << k, base, 1 << k)
            if i >> k & 1:
                mix_i += dot_nn(sb_sc[here, there], v_ref[there, span]) * cw
            else:
                dv_i += dot_nn(stb_sc[here, there], c_ref[there, span]) * cw
        mix_ref[here, span] = mix_i.astype(mix_ref.dtype)
        dv_ref[here, span] = dv_i.astype(dv_ref.dtype)


def intra(table, values, cotangent, keys, queries, grams, before, group, head_dim, cols):
    tok, width = values.shape
    groups, _, state = keys.shape
    base = min(128, tok)
    return pl.pallas_call(
        functools.partial(intra_kernel, base=base, head_dim=head_dim, group=group, cols=cols),
        grid=(width // groups // cols,),
        in_specs=[SMEM] + [VMEM] * (5 + len(before)),
        out_specs=[VMEM] * 4,
        out_shape=[pltpu.VMEM((tok, width), BF)] * 2 + [pltpu.VMEM((tok, state), F32)] * 2,
        input_output_aliases={6 + n: n for n in range(len(before))},
        scratch_shapes=[pltpu.VMEM((tok, base), F32)] * 2 + [pltpu.VMEM((tok, tok), BF)] * 2,
        compiler_params=PARAMS,
        cost_estimate=cost(4 * tok * tok * width // groups, 8 * tok * width // groups),
        name="intra",
    )(table, values, cotangent, keys, queries, grams, *before)


def near_kernel(table_ref, window_ref, p_ref, *refs, level, gate, head_dim, prior_level):
    o_ref = refs[-1]
    priors = refs[0] if len(refs) > 1 else None
    heads = o_ref.shape[0] // head_dim
    on = (lax.axis_index("seq") & 1 == gate).astype(F32)
    for h in range(heads):
        rows = blk(h, head_dim)
        out = p_ref[rows, :].astype(F32) * (weight(table_ref, h, level) * on)
        if priors is not None:
            for k in range(priors.shape[0]):
                bit = (window_ref[0] >> k & 1).astype(F32)
                out += priors[k, rows, :].astype(F32) * (weight(table_ref, h, prior_level + k) * bit)
        o_ref[rows, :] = out


def near(table, window, partner, priors, level, gate, head_dim, prior_level):
    width, state = partner.shape
    ins = [near_core(x) for x in (partner, priors) if x is not None]
    return pl.pallas_call(
        functools.partial(
            near_kernel, level=level, gate=gate, head_dim=head_dim, prior_level=prior_level
        ),
        in_specs=[SMEM, SMEM] + [VMEM] * len(ins),
        out_specs=VMEM,
        out_shape=pltpu.VMEM((width, state), F32),
        compiler_params=PARAMS,
        cost_estimate=cost(10 * width * state, 8 * width * state),
        name="near",
    )(table, window, *ins)


def combine_kernel(a_ref, b_ref, o_ref):
    half = o_ref.shape[0]
    rows = pl.ds(0, half)
    if a_ref.shape[0] > half:
        rows = pl.ds(pl.multiple_of((lax.axis_index("seq") & 1) * half, half), half)
    total = a_ref[rows, :].astype(F32) + b_ref[rows, :].astype(F32)
    o_ref[...] = total.astype(o_ref.dtype)


def combine(a, b, half):
    return pl.pallas_call(
        combine_kernel,
        in_specs=[VMEM] * 2,
        out_specs=VMEM,
        out_shape=pltpu.VMEM((half, a.shape[1]), BF),
        compiler_params=PARAMS,
        cost_estimate=cost(a.size, 4 * a.size),
        name="combine",
    )(near_core(a), near_core(b))


def far_kernel(table_ref, *refs, level, gate, head_dim, with_total):
    o_ref = refs[-1]
    partners = refs[:-2] if with_total else refs[:-1]
    half = partners[0].shape[0]
    heads = half // head_dim
    seq = lax.axis_index("seq")
    first = (seq & 1) * heads
    ons = [(seq >> (k + 1) & 1 == gate).astype(F32) for k in range(len(partners))]
    for h in range(heads):
        rows = blk(h, head_dim)
        out = None
        for k, p_ref in enumerate(partners):
            term = p_ref[rows, :].astype(F32) * (
                weight(table_ref, first + h, level + k) * ons[k]
            )
            out = term if out is None else out + term
        o_ref[rows, :] = out.astype(o_ref.dtype)
    if with_total:
        total = refs[-2][...].astype(F32) + partners[-1][...].astype(F32)
        o_ref[pl.ds(half, half), :] = total.astype(o_ref.dtype)


def far(table, partners, before, level, gate, head_dim):
    half, state = partners[0].shape
    extra = [] if before is None else [before]
    return pl.pallas_call(
        functools.partial(
            far_kernel, level=level, gate=gate, head_dim=head_dim, with_total=bool(extra)
        ),
        in_specs=[SMEM] + [VMEM] * (len(partners) + len(extra)),
        out_specs=VMEM,
        out_shape=pltpu.VMEM((half * (1 + len(extra)), state), BF),
        compiler_params=PARAMS,
        cost_estimate=cost(10 * half * state, 8 * half * state),
        name="far",
    )(table, *[near_core(x) for x in partners + extra])


def slope_kernel(near_ref, mine_ref, other_ref, x_ref, *refs, pieces):
    groups = len(refs) - pieces - 2
    g_refs, flow_ref, outs, acc = refs[:groups], refs[groups], refs[groups + 1 : -1], refs[-1]
    half = mine_ref.shape[0]
    half = flow_ref.shape[0] // 2
    core = lax.axis_index("seq") & 1
    for ref, at in ((mine_ref, core), (other_ref, 1 - core)):
        rows = pl.ds(pl.multiple_of(at * half, half), half)
        flow_ref[rows, :] = (near_ref[rows, :] + ref[pl.ds(0, half), :].astype(F32)).astype(BF)
    width = x_ref.shape[1] // groups
    for g in range(groups):
        span = slice(g * width, (g + 1) * width)
        grad = g_refs[g][...] + dot_nn(x_ref[:, span], flow_ref[span, :])
        if pieces == 1:
            outs[0][g] = grad.astype(BF)
        else:
            acc[...] = grad
            here = lax.axis_index("head")
            size = outs[0].shape[1]
            for r, out in enumerate(outs):
                rows = pl.ds(pl.multiple_of((here ^ r) * size, size), size)
                out[g] = acc[rows, :].astype(BF)


def slope(near_flow, mine, other, x, grads, pieces):
    tok, width = x.shape
    groups = len(grads)
    state = near_flow.shape[1]
    piece = (groups, tok // pieces, state)
    flow, *parts = pl.pallas_call(
        functools.partial(slope_kernel, pieces=pieces),
        in_specs=[VMEM] * (4 + groups),
        out_specs=[VMEM] * (1 + pieces),
        out_shape=[pltpu.VMEM((width, state), BF)] + [pltpu.VMEM(piece, BF)] * pieces,
        scratch_shapes=[pltpu.VMEM((tok, state), F32)],
        compiler_params=PARAMS,
        cost_estimate=cost(2 * tok * width * state, 2 * tok * width),
        name="slope",
    )(near_flow, near_core(mine), near_core(other), x, *grads)
    return flow, parts


def outs_kernel(
    table_ref, window_ref, mix_ref, q_ref, in_ref, dv_ref, k_ref, out_ref, mine_ref, other_ref,
    *refs, cols, count, head_dim, level,
):
    parts, refs = refs[:-9], refs[-9:]
    mix_hbm, dv_hbm, prior_hbm, grad_hbm, mix_sc, dv_sc, prior_sc, grad_sc, sems = refs
    _, width = mix_ref.shape
    groups = q_ref.shape[0]
    chunks = width // cols
    half = width // 2
    core = lax.axis_index("seq") & 1
    copies = []

    def send(source, target):
        copy = pltpu.make_async_copy(source, target, sems.at[len(copies)])
        copy.start()
        copies.append(copy)

    for at in range(chunks):
        rows = pl.ds(at * cols, cols)
        first = half + at * cols % half
        source = pl.ds(first, cols)
        is_mine = core == at * cols // half
        total = jnp.where(is_mine, mine_ref[source, :], other_ref[source, :]).astype(F32)
        for h in range(cols // head_dim):
            head = at * cols // head_dim + h
            piece = total[h * head_dim : (h + 1) * head_dim]
            for k in range(count):
                bit = (window_ref[0] >> k & 1).astype(F32)
                prior_sc[k, pl.ds(head * head_dim, head_dim), :] = piece * (
                    weight(table_ref, head, level + k) * bit
                )
        send(prior_sc.at[:, rows, :], prior_hbm.at[:, rows, :])
    for part, r, flow, sc, hbm in (
        (mix_ref, q_ref, in_ref, mix_sc, mix_hbm), (dv_ref, k_ref, out_ref, dv_sc, dv_hbm)
    ):
        for at in range(chunks):
            span = pl.ds(at * cols, cols)
            added = dot_nt(r[at * cols * groups // width], flow[span, :])
            sc[:, span] = (part[:, span].astype(F32) + added).astype(BF)
            send(sc.at[:, span], hbm.at[:, span])
    if parts:
        here = lax.axis_index("head")
        take = parts[0].shape[0]
        rows = parts[0].shape[1]
        stacked = grad_sc.at[0]
        for r, part in enumerate(parts):
            stacked[pl.ds((here ^ r) * take, take)] = part[...].astype(F32)
        final = grad_sc.at[1].reshape(rows, take * len(parts), parts[0].shape[2])
        final[...] = jnp.swapaxes(stacked[...], 0, 1)
        send(final, grad_hbm)
    for copy in copies:
        copy.wait()


def outs(table, window, mix, queries, inflow, dv, keys, outflow, mine, other, parts, count, level, head_dim, cols):
    tok, width = mix.shape
    state = inflow.shape[1]
    chunks = width // cols
    groups, rows = (parts[0].shape[0] * len(parts), parts[0].shape[1]) if parts else (8, 8)
    return pl.pallas_call(
        functools.partial(outs_kernel, cols=cols, count=count, head_dim=head_dim, level=level),
        in_specs=[SMEM, SMEM] + [VMEM] * (8 + len(parts)),
        out_specs=[HBM] * 4,
        out_shape=[
            pltpu.HBM((tok, width), BF), pltpu.HBM((tok, width), BF),
            pltpu.HBM((count, width, state), F32), pltpu.HBM((rows, groups, state), F32),
        ],
        scratch_shapes=[
            pltpu.VMEM((tok, width), BF), pltpu.VMEM((tok, width), BF),
            pltpu.VMEM((count, width, state), F32), pltpu.VMEM((2, groups, rows, state), F32),
            pltpu.SemaphoreType.DMA((3 * chunks + 1,)),
        ],
        compiler_params=PARAMS,
        cost_estimate=cost(4 * tok * width * state, 6 * tok * width),
        name="outs",
    )(table, window, mix, queries, inflow, dv, keys, outflow, mine, other,
      *[near_core(part) for part in parts])


def gather_kernel(*refs):
    parts, o_ref, scratch = refs[:-2], refs[-2], refs[-1]
    here = lax.axis_index("head")
    take = parts[0].shape[0]
    for r, part in enumerate(parts):
        scratch[pl.ds((here ^ r) * take, take)] = part[...].astype(F32)
    o_ref[...] = jnp.swapaxes(scratch[...], 0, 1)


def gather(parts):
    take, rows, state = parts[0].shape
    groups = take * len(parts)
    return pl.pallas_call(
        gather_kernel,
        in_specs=[VMEM] * len(parts),
        out_specs=pl.BlockSpec((rows, groups, state), lambda: (0, 0, 0)),
        out_shape=shaped((rows, groups, state), F32),
        scratch_shapes=[pltpu.VMEM((groups, rows, state), F32)],
        compiler_params=PARAMS,
        cost_estimate=cost(10**6, 6 * groups * rows * state),
        name="gather",
    )(*[near_core(part) for part in parts])


def mixer(
    values, group_keys, group_queries, level_table, window_index, prior_states, cotangent
):
    seq_count = lax.axis_size("seq")
    head_count = lax.axis_size("head")
    tok_rows = values.shape[0]
    heads_here = level_table.shape[0]
    level_table = level_table.T
    head_dim = values.shape[1] // heads_here
    state_dim = group_keys.shape[2]
    group_count = group_keys.shape[1]
    prior_count = prior_states.shape[0]
    per_group = HEADS // GROUPS
    repeats = max(1, per_group // heads_here)
    local_groups = max(1, heads_here // per_group)
    heads_local = heads_here // local_groups
    log_rows = log2(tok_rows)
    log_seq = log2(seq_count)
    log_window = log_rows + log_seq
    width = heads_here * head_dim
    half = width // 2
    pieces = head_count if head_count <= 4 and repeats == 1 else 1
    cols_in = min(4, heads_local) * head_dim
    cols = min(8, heads_here // 2) * head_dim

    def scattered(own, *sent):
        out = [own]
        for r, part in enumerate(sent):
            out.append(swap_with(part, "head", r + 1))
        return out

    def rows_of(x):
        wide = jnp.repeat(x, repeats, axis=1).swapaxes(0, 1)
        wide = wide.reshape(head_count, local_groups, -1, state_dim)
        wide = lax.all_to_all(wide, "head", split_axis=0, concat_axis=0)
        return [wide.swapaxes(0, 1).reshape(local_groups, tok_rows, state_dim)]

    if pieces == 1:
        key_parts, query_parts = rows_of(group_keys), rows_of(group_queries)
        values, cotangent = near_core(values), near_core(cotangent)
    else:
        key_parts, query_parts, values, cotangent = prep(
            group_keys, group_queries, values, cotangent, pieces
        )
        key_parts = scattered(*key_parts)
        query_parts = scattered(*query_parts)
    grams = []
    for g in range(local_groups):
        grams.append(
            gram(level_table, values, cotangent, g, local_groups, head_dim, cols_in)
        )

    def exchange(own, gate, priors):
        partner = swap_with(own, "seq", 1)
        near_flow = near(
            level_table, window_index, partner, priors, 1 + log_rows, gate, head_dim,
            1 + log_window,
        )
        total = combine(own, partner, half)
        partners = []
        for bit in range(1, log_seq):
            partners.append(swap_with(total, "seq", 1 << bit))
            if bit < log_seq - 1:
                total = combine(total, partners[-1], half)
        before = None if priors is not None else total
        mine = far(level_table, partners, before, 2 + log_rows, gate, head_dim)
        other = swap_with(mine, "seq", 1)
        return near_flow, mine, other

    states, key_rows = block_states(values, key_parts)
    priors = prior_states.reshape(prior_count, width, state_dim)
    in_near, in_mine, in_other = exchange(states, 1, priors)
    adjoints, query_rows = block_states(cotangent, query_parts)
    out_near, out_mine, out_other = exchange(adjoints, 0, None)
    parts, query_grads, key_grads = [], [], []
    for g in range(local_groups):
        *parts, query_grad, key_grad = intra(
            level_table, values, cotangent, key_rows, query_rows, grams[g], parts, g,
            head_dim, cols_in,
        )
        query_grads.append(query_grad)
        key_grads.append(key_grad)
    mix_part, dv_part = parts

    def back(part):
        part = part.reshape(local_groups, head_count, -1, state_dim).swapaxes(0, 1)
        part = lax.all_to_all(part, "head", split_axis=0, concat_axis=0).astype(F32)
        part = part.reshape(group_count, repeats, -1, state_dim).sum(axis=1)
        return part.swapaxes(0, 1)

    inflow, query_parts = slope(in_near, in_mine, in_other, cotangent, query_grads, pieces)
    outflow, key_parts = slope(out_near, out_mine, out_other, values, key_grads, pieces)
    if pieces > 1:
        query_parts = scattered(*query_parts)
        key_parts = scattered(*key_parts)
    mixer_out, grad_values, grad_prior, grad_queries = outs(
        level_table, window_index, mix_part, query_rows, inflow, dv_part, key_rows, outflow,
        out_mine, out_other, query_parts if pieces > 1 else [], prior_count, 1 + log_window,
        head_dim, cols,
    )
    if pieces > 1:
        grad_keys = gather(key_parts)
    else:
        grad_queries, grad_keys = back(query_parts[0]), back(key_parts[0])
    return (mixer_out, grad_values, grad_keys, grad_queries, grad_prior.reshape(prior_states.shape))


def solution(mesh):
    placed = (
        P("seq", "head"),
        P(("seq", "head"), None, None),
        P(("seq", "head"), None, None),
        P("head", None),
        P(),
        P(None, "head", None, None),
        P("seq", "head"),
    )
    return jax.shard_map(
        mixer,
        mesh=mesh,
        in_specs=placed,
        out_specs=(
            P("seq", "head"),
            P("seq", "head"),
            P(("seq", "head"), None, None),
            P(("seq", "head"), None, None),
            P(None, "head", None, None),
        ),
        check_vma=False,
    )
```

```python
import functools

import jax
import jax.numpy as jnp
from jax import lax
from jax.experimental import pallas as pl
from jax.experimental.pallas import tpu as pltpu
from jax.sharding import PartitionSpec as P


HEADS = 128
GROUPS = 8
BF = jnp.bfloat16
F32 = jnp.float32
SMEM = pl.BlockSpec(memory_space=pltpu.SMEM)
VMEM = pl.BlockSpec(memory_space=pltpu.VMEM)
HBM = pl.BlockSpec(memory_space=pltpu.HBM)
PARAMS = pltpu.CompilerParams(vmem_limit_bytes=24 << 20)


def near_core(array):
    return pltpu.with_memory_space_constraint(array, pltpu.VMEM)


def far_off(array):
    return pltpu.with_memory_space_constraint(array, pltpu.HBM)


def swap_with(array, axis, mask):
    return lax.ppermute(array, axis, [(i, i ^ mask) for i in range(lax.axis_size(axis))])


def dot_nn(a, b):
    return lax.dot_general(a, b, (((1,), (0,)), ((), ())), preferred_element_type=F32)


def dot_nt(a, b):
    return lax.dot_general(a, b, (((1,), (1,)), ((), ())), preferred_element_type=F32)


def dot_tn(a, b):
    return lax.dot_general(a, b, (((0,), (0,)), ((), ())), preferred_element_type=F32)


def shaped(shape, dtype):
    return jax.ShapeDtypeStruct(shape, dtype)


def cost(flops, bytes_accessed):
    return pl.CostEstimate(flops=flops, transcendentals=0, bytes_accessed=bytes_accessed)


def weight(table_ref, head, level):
    return table_ref[level, head].astype(F32) * 2.0 ** (-max(level - 1, 0) / 2)


def log2(number):
    return number.bit_length() - 1


def prep_kernel(*refs, pieces):
    x_refs, big, refs = refs[:2], refs[2:4], refs[4:]
    outs, big_outs = refs[: 2 * pieces], refs[2 * pieces : 2 * pieces + 2]
    raw, scratch, sems = refs[2 * pieces + 2 :]
    here = lax.axis_index("head")
    copies = [pltpu.make_async_copy(x, raw.at[n], sems.at[n]) for n, x in enumerate(x_refs)]
    copies += [
        pltpu.make_async_copy(x, out, sems.at[2 + n])
        for n, (x, out) in enumerate(zip(big, big_outs))
    ]
    for copy in copies:
        copy.start()
    for n in range(2):
        copies[n].wait()
        scratch[...] = jnp.swapaxes(raw[n].astype(F32), 0, 1)
        for r, out in enumerate(outs[n * pieces : (n + 1) * pieces]):
            take = out.shape[0]
            out[...] = scratch[pl.ds((here ^ r) * take, take)].astype(out.dtype)
    copies[2].wait()
    copies[3].wait()


def prep(keys, queries, values, cotangent, pieces):
    rows, groups, state = keys.shape
    out = pl.pallas_call(
        functools.partial(prep_kernel, pieces=pieces),
        in_specs=[HBM] * 4,
        out_specs=[VMEM] * (2 * pieces + 2),
        out_shape=[pltpu.VMEM((groups // pieces, rows, state), BF)] * (2 * pieces)
        + [pltpu.VMEM(values.shape, BF)] * 2,
        scratch_shapes=[
            pltpu.VMEM((2,) + keys.shape, BF),
            pltpu.VMEM((groups, rows, state), F32),
            pltpu.SemaphoreType.DMA((4,)),
        ],
        compiler_params=PARAMS,
        cost_estimate=cost(10**6, 8 * keys.size),
        name="prep",
    )(*[far_off(x) for x in (keys, queries, values, cotangent)])
    return out[:pieces], out[pieces : 2 * pieces], out[-2], out[-1]


def states_kernel(x_ref, *refs):
    parts, (o_ref, rows_ref) = refs[:-2], refs[-2:]
    if len(parts) == 1:
        rows_ref[...] = parts[0][...]
    else:
        here = lax.axis_index("head")
        size = parts[0].shape[1]
        for r, part in enumerate(parts):
            rows_ref[:, pl.ds(pl.multiple_of((here ^ r) * size, size), size), :] = part[...]
    groups = rows_ref.shape[0]
    width = x_ref.shape[1] // groups
    for g in range(groups):
        span = slice(g * width, (g + 1) * width)
        o_ref[span, :] = dot_tn(rows_ref[g], x_ref[:, span]).T.astype(o_ref.dtype)


def block_states(x, parts):
    tok, width = x.shape
    lg, _, state = parts[0].shape
    return pl.pallas_call(
        states_kernel,
        in_specs=[VMEM] * (1 + len(parts)),
        out_specs=[VMEM] * 2,
        out_shape=[pltpu.VMEM((width, state), BF), pltpu.VMEM((lg, tok, state), BF)],
        compiler_params=PARAMS,
        cost_estimate=cost(2 * tok * width * state, 2 * tok * width),
        name="states",
    )(x, *[near_core(part) for part in parts])


def spread_grid(base):
    rows = lax.broadcasted_iota(jnp.int32, (base, base), 0)
    cols = lax.broadcasted_iota(jnp.int32, (base, base), 1)
    return rows, cols, rows ^ cols


def factor_of(table_ref, head, spread, base):
    out = jnp.full((base, base), weight(table_ref, head, 0), F32)
    for level in range(1, log2(base) + 1):
        out = jnp.where(spread >= 1 << (level - 1), weight(table_ref, head, level), out)
    return out


def sides(base, head_dim):
    lane = lax.broadcasted_iota(jnp.int32, (base, 2 * head_dim), 1)
    return lane < head_dim, (lane < head_dim).astype(BF), (lane >= head_dim).astype(BF)


def blk(i, base, n=1):
    return pl.ds(i * base, n * base)


def pair_weights(table_ref, first_head, pairs, level, is_left):
    rows = [
        jnp.where(
            is_left,
            weight(table_ref, first_head + 2 * p, level),
            weight(table_ref, first_head + 2 * p + 1, level),
        )
        for p in range(pairs)
    ]
    return jnp.concatenate(rows, axis=1)


def gram_kernel(table_ref, v_ref, c_ref, g_ref, g_sc, *, base, head_dim, group, cols):
    tok = v_ref.shape[0]
    blocks = tok // base
    heads = cols // head_dim
    first_head = group * heads
    first_col = group * cols
    rows_i, cols_i, spread = spread_grid(base)
    is_left, left, right = sides(base, head_dim)

    g_sc[...] = jnp.zeros_like(g_sc)

    for pair in range(heads // 2):
        span = pl.ds(first_col + pair * 2 * head_dim, 2 * head_dim)
        f_a = factor_of(table_ref, first_head + 2 * pair, spread, base)
        f_b = factor_of(table_ref, first_head + 2 * pair + 1, spread, base)
        for i in range(blocks):
            v_i, c_i = v_ref[blk(i, base), span], c_ref[blk(i, base), span]
            raw = dot_nt(c_i, jnp.concatenate([v_i * left, v_i * right], axis=0))
            g_sc[blk(i, base), blk(i, base)] += f_a * raw[:, :base] + f_b * raw[:, base:]
    span = pl.ds(first_col, cols)
    for k in range(log2(blocks)):
        cw = pair_weights(table_ref, first_head, heads // 2, log2(base) + 1 + k, is_left[:1])
        for i in range(blocks):
            if i >> k & 1:
                there = blk((i >> k ^ 1) << k, base, 1 << k)
                scaled = (c_ref[blk(i, base), span].astype(F32) * cw).astype(BF)
                g_sc[blk(i, base), there] += dot_nt(scaled, v_ref[there, span])

    for i in range(blocks):
        here = blk(i, base)
        g_sc[here, here] = jnp.where(rows_i >= cols_i, g_sc[here, here], 0.0)
    g_ref[...] = g_sc[...].astype(BF)


def gram(table, values, cotangent, group, groups, head_dim, cols):
    tok, width = values.shape
    base = min(128, tok)
    return pl.pallas_call(
        functools.partial(gram_kernel, base=base, head_dim=head_dim, group=group, cols=cols),
        in_specs=[SMEM, VMEM, VMEM],
        out_specs=VMEM,
        out_shape=pltpu.VMEM((tok, tok), BF),
        scratch_shapes=[pltpu.VMEM((tok, tok), F32)],
        compiler_params=PARAMS,
        cost_estimate=cost(2 * tok * tok * width // groups, 4 * tok * width // groups),
        name="gram",
    )(table, values, cotangent)


def intra_kernel(table_ref, v_ref, c_ref, kg_rows, qg_rows, g_ref, *refs, base, head_dim, group, cols):
    mix_ref, dv_ref, qg_ref, kg_ref, s_sc, st_sc, sb_sc, stb_sc = refs[-8:]
    k_ref, q_ref = kg_rows.at[group], qg_rows.at[group]
    tok = v_ref.shape[0]
    blocks = tok // base
    heads = cols // head_dim
    first_head = group * heads
    first_col = group * cols
    rows_i, cols_i, spread = spread_grid(base)
    is_left, left, right = sides(base, head_dim)

    for i in range(blocks):
        here = blk(i, base)
        q_i, k_i = q_ref[here, :], k_ref[here, :]
        s_sc[here, :] = jnp.where(rows_i >= cols_i, dot_nt(q_i, k_i), 0.0)
        st_sc[here, :] = jnp.where(rows_i <= cols_i, dot_nt(k_i, q_i), 0.0)
        above = blk(0, base, i)
        rest = blk(i + 1, base, blocks - 1 - i)
        if i > 0:
            sb_sc[here, above] = dot_nt(q_i, k_ref[above, :]).astype(BF)
        if i < blocks - 1:
            stb_sc[here, rest] = dot_nt(k_i, q_ref[rest, :]).astype(BF)
        until = blk(0, base, i + 1)
        below = blk(i, base, blocks - i)
        qg_ref[here, :] = dot_nn(g_ref[here, until], k_ref[until, :])
        kg_ref[here, :] = dot_tn(g_ref[below, here], q_ref[below, :])

    mix = [[] for _ in range(blocks)]
    dv = [[] for _ in range(blocks)]
    for pair in range(heads // 2):
        span = pl.ds(first_col + pair * 2 * head_dim, 2 * head_dim)
        f_a = factor_of(table_ref, first_head + 2 * pair, spread, base)
        f_b = factor_of(table_ref, first_head + 2 * pair + 1, spread, base)
        for i in range(blocks):
            here = blk(i, base)
            for f_ref, x_ref, out in ((s_sc, v_ref, mix), (st_sc, c_ref, dv)):
                s_i, x_i = f_ref[here, :], x_ref[here, span]
                w_cat = jnp.concatenate([(f_a * s_i).astype(BF), (f_b * s_i).astype(BF)], axis=1)
                stacked = jnp.concatenate([x_i * left, x_i * right], axis=0)
                out[i].append(dot_nn(w_cat, stacked))
    scales = [
        pair_weights(table_ref, first_head, heads // 2, log2(base) + 1 + k, is_left[:1])
        for k in range(log2(blocks))
    ]
    span = pl.ds(first_col, cols)
    for i in range(blocks):
        here = blk(i, base)
        mix_i = jnp.concatenate(mix[i], axis=1)
        dv_i = jnp.concatenate(dv[i], axis=1)
        for k, cw in enumerate(scales):
            there = blk((i >> k ^ 1) << k, base, 1 << k)
            if i >> k & 1:
                mix_i += dot_nn(sb_sc[here, there], v_ref[there, span]) * cw
            else:
                dv_i += dot_nn(stb_sc[here, there], c_ref[there, span]) * cw
        mix_ref[here, span] = mix_i.astype(mix_ref.dtype)
        dv_ref[here, span] = dv_i.astype(dv_ref.dtype)


def intra(table, values, cotangent, keys, queries, grams, before, group, head_dim, cols):
    tok, width = values.shape
    groups, _, state = keys.shape
    base = min(128, tok)
    return pl.pallas_call(
        functools.partial(intra_kernel, base=base, head_dim=head_dim, group=group, cols=cols),
        in_specs=[SMEM] + [VMEM] * (5 + len(before)),
        out_specs=[VMEM] * 4,
        out_shape=[pltpu.VMEM((tok, width), BF)] * 2 + [pltpu.VMEM((tok, state), F32)] * 2,
        input_output_aliases={6 + n: n for n in range(len(before))},
        scratch_shapes=[pltpu.VMEM((tok, base), F32)] * 2 + [pltpu.VMEM((tok, tok), BF)] * 2,
        compiler_params=PARAMS,
        cost_estimate=cost(4 * tok * tok * width // groups, 8 * tok * width // groups),
        name="intra",
    )(table, values, cotangent, keys, queries, grams, *before)


def near_kernel(table_ref, window_ref, p_ref, *refs, level, gate, head_dim, prior_level):
    o_ref = refs[-1]
    priors = refs[0] if len(refs) > 1 else None
    heads = o_ref.shape[0] // head_dim
    on = (lax.axis_index("seq") & 1 == gate).astype(F32)
    for h in range(heads):
        rows = blk(h, head_dim)
        out = p_ref[rows, :].astype(F32) * (weight(table_ref, h, level) * on)
        if priors is not None:
            for k in range(priors.shape[0]):
                bit = (window_ref[0] >> k & 1).astype(F32)
                out += priors[k, rows, :].astype(F32) * (weight(table_ref, h, prior_level + k) * bit)
        o_ref[rows, :] = out


def near(table, window, partner, priors, level, gate, head_dim, prior_level):
    width, state = partner.shape
    ins = [near_core(x) for x in (partner, priors) if x is not None]
    return pl.pallas_call(
        functools.partial(
            near_kernel, level=level, gate=gate, head_dim=head_dim, prior_level=prior_level
        ),
        in_specs=[SMEM, SMEM] + [VMEM] * len(ins),
        out_specs=VMEM,
        out_shape=pltpu.VMEM((width, state), F32),
        compiler_params=PARAMS,
        cost_estimate=cost(10 * width * state, 8 * width * state),
        name="near",
    )(table, window, *ins)


def combine_kernel(a_ref, b_ref, o_ref):
    half = o_ref.shape[0]
    rows = pl.ds(0, half)
    if a_ref.shape[0] > half:
        rows = pl.ds(pl.multiple_of((lax.axis_index("seq") & 1) * half, half), half)
    total = a_ref[rows, :].astype(F32) + b_ref[rows, :].astype(F32)
    o_ref[...] = total.astype(o_ref.dtype)


def combine(a, b, half):
    return pl.pallas_call(
        combine_kernel,
        in_specs=[VMEM] * 2,
        out_specs=VMEM,
        out_shape=pltpu.VMEM((half, a.shape[1]), BF),
        compiler_params=PARAMS,
        cost_estimate=cost(a.size, 4 * a.size),
        name="combine",
    )(near_core(a), near_core(b))


def far_kernel(table_ref, *refs, level, gate, head_dim, with_total):
    o_ref = refs[-1]
    partners = refs[:-2] if with_total else refs[:-1]
    half = partners[0].shape[0]
    heads = half // head_dim
    seq = lax.axis_index("seq")
    first = (seq & 1) * heads
    ons = [(seq >> (k + 1) & 1 == gate).astype(F32) for k in range(len(partners))]
    for h in range(heads):
        rows = blk(h, head_dim)
        out = None
        for k, p_ref in enumerate(partners):
            term = p_ref[rows, :].astype(F32) * (
                weight(table_ref, first + h, level + k) * ons[k]
            )
            out = term if out is None else out + term
        o_ref[rows, :] = out.astype(o_ref.dtype)
    if with_total:
        total = refs[-2][...].astype(F32) + partners[-1][...].astype(F32)
        o_ref[pl.ds(half, half), :] = total.astype(o_ref.dtype)


def far(table, partners, before, level, gate, head_dim):
    half, state = partners[0].shape
    extra = [] if before is None else [before]
    return pl.pallas_call(
        functools.partial(
            far_kernel, level=level, gate=gate, head_dim=head_dim, with_total=bool(extra)
        ),
        in_specs=[SMEM] + [VMEM] * (len(partners) + len(extra)),
        out_specs=VMEM,
        out_shape=pltpu.VMEM((half * (1 + len(extra)), state), BF),
        compiler_params=PARAMS,
        cost_estimate=cost(10 * half * state, 8 * half * state),
        name="far",
    )(table, *[near_core(x) for x in partners + extra])


def slope_kernel(near_ref, mine_ref, other_ref, x_ref, *refs, pieces):
    groups = len(refs) - pieces - 2
    g_refs, flow_ref, outs, acc = refs[:groups], refs[groups], refs[groups + 1 : -1], refs[-1]
    half = mine_ref.shape[0]
    half = flow_ref.shape[0] // 2
    core = lax.axis_index("seq") & 1
    for ref, at in ((mine_ref, core), (other_ref, 1 - core)):
        rows = pl.ds(pl.multiple_of(at * half, half), half)
        flow_ref[rows, :] = (near_ref[rows, :] + ref[pl.ds(0, half), :].astype(F32)).astype(BF)
    width = x_ref.shape[1] // groups
    for g in range(groups):
        span = slice(g * width, (g + 1) * width)
        grad = g_refs[g][...] + dot_nn(x_ref[:, span], flow_ref[span, :])
        if pieces == 1:
            outs[0][g] = grad.astype(BF)
        else:
            acc[...] = grad
            here = lax.axis_index("head")
            size = outs[0].shape[1]
            for r, out in enumerate(outs):
                rows = pl.ds(pl.multiple_of((here ^ r) * size, size), size)
                out[g] = acc[rows, :].astype(BF)


def slope(near_flow, mine, other, x, grads, pieces):
    tok, width = x.shape
    groups = len(grads)
    state = near_flow.shape[1]
    piece = (groups, tok // pieces, state)
    flow, *parts = pl.pallas_call(
        functools.partial(slope_kernel, pieces=pieces),
        in_specs=[VMEM] * (4 + groups),
        out_specs=[VMEM] * (1 + pieces),
        out_shape=[pltpu.VMEM((width, state), BF)] + [pltpu.VMEM(piece, BF)] * pieces,
        scratch_shapes=[pltpu.VMEM((tok, state), F32)],
        compiler_params=PARAMS,
        cost_estimate=cost(2 * tok * width * state, 2 * tok * width),
        name="slope",
    )(near_flow, near_core(mine), near_core(other), x, *grads)
    return flow, parts


def outs_kernel(
    table_ref, window_ref, mix_ref, q_ref, in_ref, dv_ref, k_ref, out_ref, mine_ref, other_ref,
    *refs, cols, count, head_dim, level,
):
    parts, refs = refs[:-9], refs[-9:]
    mix_hbm, dv_hbm, prior_hbm, grad_hbm, mix_sc, dv_sc, prior_sc, grad_sc, sems = refs
    _, width = mix_ref.shape
    groups = q_ref.shape[0]
    chunks = width // cols
    half = width // 2
    core = lax.axis_index("seq") & 1
    copies = []

    def send(source, target):
        copy = pltpu.make_async_copy(source, target, sems.at[len(copies)])
        copy.start()
        copies.append(copy)

    for at in range(chunks):
        rows = pl.ds(at * cols, cols)
        first = half + at * cols % half
        source = pl.ds(first, cols)
        is_mine = core == at * cols // half
        total = jnp.where(is_mine, mine_ref[source, :], other_ref[source, :]).astype(F32)
        for h in range(cols // head_dim):
            head = at * cols // head_dim + h
            piece = total[h * head_dim : (h + 1) * head_dim]
            for k in range(count):
                bit = (window_ref[0] >> k & 1).astype(F32)
                prior_sc[k, pl.ds(head * head_dim, head_dim), :] = piece * (
                    weight(table_ref, head, level + k) * bit
                )
        send(prior_sc.at[:, rows, :], prior_hbm.at[:, rows, :])
    for part, r, flow, sc, hbm in (
        (mix_ref, q_ref, in_ref, mix_sc, mix_hbm), (dv_ref, k_ref, out_ref, dv_sc, dv_hbm)
    ):
        for at in range(chunks):
            span = pl.ds(at * cols, cols)
            added = dot_nt(r[at * cols * groups // width], flow[span, :])
            sc[:, span] = (part[:, span].astype(F32) + added).astype(BF)
            send(sc.at[:, span], hbm.at[:, span])
    if parts:
        here = lax.axis_index("head")
        take = parts[0].shape[0]
        rows = parts[0].shape[1]
        stacked = grad_sc.at[0]
        for r, part in enumerate(parts):
            stacked[pl.ds((here ^ r) * take, take)] = part[...].astype(F32)
        final = grad_sc.at[1].reshape(rows, take * len(parts), parts[0].shape[2])
        final[...] = jnp.swapaxes(stacked[...], 0, 1)
        send(final, grad_hbm)
    for copy in copies:
        copy.wait()


def outs(table, window, mix, queries, inflow, dv, keys, outflow, mine, other, parts, count, level, head_dim, cols):
    tok, width = mix.shape
    state = inflow.shape[1]
    chunks = width // cols
    groups, rows = (parts[0].shape[0] * len(parts), parts[0].shape[1]) if parts else (8, 8)
    return pl.pallas_call(
        functools.partial(outs_kernel, cols=cols, count=count, head_dim=head_dim, level=level),
        in_specs=[SMEM, SMEM] + [VMEM] * (8 + len(parts)),
        out_specs=[HBM] * 4,
        out_shape=[
            pltpu.HBM((tok, width), BF), pltpu.HBM((tok, width), BF),
            pltpu.HBM((count, width, state), F32), pltpu.HBM((rows, groups, state), F32),
        ],
        scratch_shapes=[
            pltpu.VMEM((tok, width), BF), pltpu.VMEM((tok, width), BF),
            pltpu.VMEM((count, width, state), F32), pltpu.VMEM((2, groups, rows, state), F32),
            pltpu.SemaphoreType.DMA((3 * chunks + 1,)),
        ],
        compiler_params=PARAMS,
        cost_estimate=cost(4 * tok * width * state, 6 * tok * width),
        name="outs",
    )(table, window, mix, queries, inflow, dv, keys, outflow, mine, other,
      *[near_core(part) for part in parts])


def gather_kernel(*refs):
    parts, o_ref, scratch = refs[:-2], refs[-2], refs[-1]
    here = lax.axis_index("head")
    take = parts[0].shape[0]
    for r, part in enumerate(parts):
        scratch[pl.ds((here ^ r) * take, take)] = part[...].astype(F32)
    o_ref[...] = jnp.swapaxes(scratch[...], 0, 1)


def gather(parts):
    take, rows, state = parts[0].shape
    groups = take * len(parts)
    return pl.pallas_call(
        gather_kernel,
        in_specs=[VMEM] * len(parts),
        out_specs=pl.BlockSpec((rows, groups, state), lambda: (0, 0, 0)),
        out_shape=shaped((rows, groups, state), F32),
        scratch_shapes=[pltpu.VMEM((groups, rows, state), F32)],
        compiler_params=PARAMS,
        cost_estimate=cost(10**6, 6 * groups * rows * state),
        name="gather",
    )(*[near_core(part) for part in parts])


def mixer(
    values, group_keys, group_queries, level_table, window_index, prior_states, cotangent
):
    seq_count = lax.axis_size("seq")
    head_count = lax.axis_size("head")
    tok_rows = values.shape[0]
    heads_here = level_table.shape[0]
    level_table = level_table.T
    head_dim = values.shape[1] // heads_here
    state_dim = group_keys.shape[2]
    group_count = group_keys.shape[1]
    prior_count = prior_states.shape[0]
    per_group = HEADS // GROUPS
    repeats = max(1, per_group // heads_here)
    local_groups = max(1, heads_here // per_group)
    heads_local = heads_here // local_groups
    log_rows = log2(tok_rows)
    log_seq = log2(seq_count)
    log_window = log_rows + log_seq
    width = heads_here * head_dim
    half = width // 2
    pieces = head_count if head_count <= 4 and repeats == 1 else 1
    cols_in = heads_local * head_dim
    cols = min(8, heads_here // 2) * head_dim

    def scattered(own, *sent):
        out = [own]
        for r, part in enumerate(sent):
            out.append(swap_with(part, "head", r + 1))
        return out

    def rows_of(x):
        wide = jnp.repeat(x, repeats, axis=1).swapaxes(0, 1)
        wide = wide.reshape(head_count, local_groups, -1, state_dim)
        wide = lax.all_to_all(wide, "head", split_axis=0, concat_axis=0)
        return [wide.swapaxes(0, 1).reshape(local_groups, tok_rows, state_dim)]

    if pieces == 1:
        key_parts, query_parts = rows_of(group_keys), rows_of(group_queries)
        values, cotangent = near_core(values), near_core(cotangent)
    else:
        key_parts, query_parts, values, cotangent = prep(
            group_keys, group_queries, values, cotangent, pieces
        )
        key_parts = scattered(*key_parts)
        query_parts = scattered(*query_parts)
    grams = []
    for g in range(local_groups):
        grams.append(
            gram(level_table, values, cotangent, g, local_groups, head_dim, cols_in)
        )

    def exchange(own, gate, priors):
        partner = swap_with(own, "seq", 1)
        near_flow = near(
            level_table, window_index, partner, priors, 1 + log_rows, gate, head_dim,
            1 + log_window,
        )
        total = combine(own, partner, half)
        partners = []
        for bit in range(1, log_seq):
            partners.append(swap_with(total, "seq", 1 << bit))
            if bit < log_seq - 1:
                total = combine(total, partners[-1], half)
        before = None if priors is not None else total
        mine = far(level_table, partners, before, 2 + log_rows, gate, head_dim)
        other = swap_with(mine, "seq", 1)
        return near_flow, mine, other

    states, key_rows = block_states(values, key_parts)
    priors = prior_states.reshape(prior_count, width, state_dim)
    in_near, in_mine, in_other = exchange(states, 1, priors)
    adjoints, query_rows = block_states(cotangent, query_parts)
    out_near, out_mine, out_other = exchange(adjoints, 0, None)
    parts, query_grads, key_grads = [], [], []
    for g in range(local_groups):
        *parts, query_grad, key_grad = intra(
            level_table, values, cotangent, key_rows, query_rows, grams[g], parts, g,
            head_dim, cols_in,
        )
        query_grads.append(query_grad)
        key_grads.append(key_grad)
    mix_part, dv_part = parts

    def back(part):
        part = part.reshape(local_groups, head_count, -1, state_dim).swapaxes(0, 1)
        part = lax.all_to_all(part, "head", split_axis=0, concat_axis=0).astype(F32)
        part = part.reshape(group_count, repeats, -1, state_dim).sum(axis=1)
        return part.swapaxes(0, 1)

    inflow, query_parts = slope(in_near, in_mine, in_other, cotangent, query_grads, pieces)
    outflow, key_parts = slope(out_near, out_mine, out_other, values, key_grads, pieces)
    if pieces > 1:
        query_parts = scattered(*query_parts)
        key_parts = scattered(*key_parts)
    mixer_out, grad_values, grad_prior, grad_queries = outs(
        level_table, window_index, mix_part, query_rows, inflow, dv_part, key_rows, outflow,
        out_mine, out_other, query_parts if pieces > 1 else [], prior_count, 1 + log_window,
        head_dim, cols,
    )
    if pieces > 1:
        grad_keys = gather(key_parts)
    else:
        grad_queries, grad_keys = back(query_parts[0]), back(key_parts[0])
    return (mixer_out, grad_values, grad_keys, grad_queries, grad_prior.reshape(prior_states.shape))


def solution(mesh):
    placed = (
        P("seq", "head"),
        P(("seq", "head"), None, None),
        P(("seq", "head"), None, None),
        P("head", None),
        P(),
        P(None, "head", None, None),
        P("seq", "head"),
    )
    return jax.shard_map(
        mixer,
        mesh=mesh,
        in_specs=placed,
        out_specs=(
            P("seq", "head"),
            P("seq", "head"),
            P(("seq", "head"), None, None),
            P(("seq", "head"), None, None),
            P(None, "head", None, None),
        ),
        check_vma=False,
    )
```
